32 devices in a mesh: cosmo: 2 (over y), shell: 4 (over x, core), band: 4 (over z).
Axes of the slice: x: 2, y: 2, z: 4, core: 2. Of those that a mesh axis runs over, the one named last changes fastest.
Arguments:
- cycle_modes: float32 [1024, 16, 2, 16], P(('cosmo', 'shell'), 'band'), parts along dimension 0, may hold values from -6 to 6
- cycle_weight: float32 [16], P('band'), may hold values from 0.5 to 2
- legendre: float32 [16, 16, 4096], P('band'), may hold values from -1.5 to 1.5
- spin_plus: bfloat16 [16, 16, 4096], P('band'), may hold values from -1.5 to 1.5
- spin_minus: bfloat16 [16, 16, 4096], P('band'), may hold values from -1.5 to 1.5
- window: float32 [512, 4096], P('shell'), may hold values from 0.3 to 3
- lensing: float32 [1024], P(('cosmo', 'shell')), parts along dimension 0, may hold values from 0.05 to 0.5
- source_shell: int32 [8], P('cosmo'), parts along dimension 0, may hold values from 384 to 511
Outputs:
- lensing_maps: float32 [8, 3, 16, 2, 16], P(('cosmo', 'shell'), None, 'band'), parts along dimension 0
The draws below stay inside these ranges and needn't reach their ends.
There are 2 independent parts, one for each index of `cosmo`. The reference program is written for one: setup_inputs(seed, part) draws one part's arguments, and reference() takes and returns one part's arrays. A program takes and returns all parts, laid end to end along the dimension named above; an argument that names none is the same for every part. Nothing has to cross between parts.
All inputs are finite; a program needn't handle non-finite values.
Results may differ from the reference program's by a relative error of at most 0.00073.
Values sent between devices are 32-bit elements; how exact they have to be, the bound alone decides.
No kernel may reach another device: no remote copies, remote signals or barrier semaphores. Data moves between devices by JAX's collectives and lax.ppermute only.
A program may use at most 64 MiB of HBM per device.

```python
import math
import jax
import jax.numpy as jnp
from jax import lax

L = 4096
BINS = 4
SH_DEV = 128
SHELLS = 512
CYCLES = 16
ORDERS = 16
N_SHELL = 4


def with_ends(array, stream_key, smallest, largest):
    dims = array.shape
    index_at = [jax.random.randint(jax.random.fold_in(stream_key, axis), (), 0, dims[axis]) for axis in range(len(dims))]
    array = array.at[tuple(index_at)].set(smallest)
    longest = dims.index(max(dims))
    index_at[longest] = (index_at[longest] + 1) % dims[longest]
    return array.at[tuple(index_at)].set(largest)


def steps_of(key, extent, split, least, largest):
    factor_of = 1.0
    for axis_at, parts in split:
        draws = jax.random.uniform(jax.random.fold_in(jax.random.fold_in(key, 6), axis_at), (parts,), jnp.float32, least / len(split), largest / len(split))
        factor_of = factor_of * jnp.repeat(jnp.exp(draws), extent[axis_at] // parts).reshape((-1,) + (1,) * (len(extent) - 1 - axis_at))
    return factor_of


def gaussian(key, shape, spread, bound, split=(), kind=jnp.bfloat16):
    result = spread * jax.random.normal(key, shape, jnp.float32)
    if split:
        result = result * steps_of(key, shape, split, -0.22, 0.18)
    return jnp.clip(result, -bound, bound).astype(kind)


def setup_inputs(seed: int = 0, part: int = 0) -> dict:
    arg_keys = jax.random.split(jax.random.key(seed), 9)
    part_keys = jax.random.split(jax.random.fold_in(arg_keys[8], part), 9)
    cycle_modes = gaussian(part_keys[0], (SHELLS, CYCLES, 2, ORDERS), 1.0, 6.0, ((0, 4), (1, 4)), jnp.float32)
    cycle_weight = jnp.clip(jnp.exp(math.log(2.0) - 1.3862944 * jax.random.uniform(arg_keys[1], (CYCLES,), jnp.float32) ** steps_of(arg_keys[1], (CYCLES,), ((0, 4),), -0.2, 0.2)), 0.5, 2.0)
    legendre = gaussian(arg_keys[2], (ORDERS, CYCLES, L), CYCLES ** -0.5, 1.5, ((0, 4),), jnp.float32)
    spin_plus = gaussian(arg_keys[3], (ORDERS, CYCLES, L), CYCLES ** -0.5, 1.5, ((0, 4),))
    spin_minus = gaussian(arg_keys[4], (ORDERS, CYCLES, L), CYCLES ** -0.5, 1.5, ((0, 4),))
    window = jnp.clip(jnp.exp(math.log(3.0) - 2.3025851 * jax.random.uniform(arg_keys[5], (SHELLS, L), jnp.float32) ** steps_of(arg_keys[5], (SHELLS, L), ((0, 4),), -0.2, 0.2)), 0.3, 3.0)
    lensing = jnp.clip(jnp.exp(math.log(0.5) - 2.3025851 * jax.random.uniform(part_keys[6], (SHELLS,), jnp.float32) ** steps_of(part_keys[6], (SHELLS,), ((0, 4),), -0.2, 0.2)), 0.05, 0.5)
    source_shell = with_ends(jax.random.randint(part_keys[7], (BINS,), 3 * SHELLS // 4, SHELLS), jax.random.fold_in(part_keys[7], 1), 3 * SHELLS // 4, SHELLS - 1).astype(jnp.int32)
    return dict(cycle_modes=cycle_modes, cycle_weight=cycle_weight, legendre=legendre, spin_plus=spin_plus, spin_minus=spin_minus, window=window, lensing=lensing, source_shell=source_shell)


def reference(cycle_modes, cycle_weight, legendre, spin_plus, spin_minus, window, lensing, source_shell):
    highest = lax.Precision.HIGHEST
    weighted = cycle_modes * cycle_weight[None, :, None, None]
    degree = jnp.arange(L).astype(jnp.float32)
    shell_ids = jnp.arange(SHELLS).astype(jnp.int32)
    source = source_shell.astype(jnp.int32)
    efficiency = lensing[None, :] * jnp.maximum(source[:, None] - shell_ids[None, :], 0).astype(jnp.float32) / (source[:, None] + 1).astype(jnp.float32)
    shear_ratio = jnp.where(degree >= 2.0, jnp.sqrt((degree + 2.0) * (degree - 1.0) / jnp.maximum(degree * (degree + 1.0), 1.0)), 0.0)
    plus_table = spin_plus.astype(jnp.float32)
    minus_table = spin_minus.astype(jnp.float32)
    summed = jnp.zeros((BINS, 3, CYCLES, 2, ORDERS), jnp.float32)
    for group in range(N_SHELL):
        first = group * SH_DEV
        harmonic = jnp.einsum('srcm,mrl->smcl', weighted[first:first + SH_DEV], legendre, precision=highest)
        factor = window[first:first + SH_DEV][:, None, None, :]
        binned = jnp.einsum('bs,smcl->bmcl', efficiency[:, first:first + SH_DEV], harmonic * factor, precision=highest)
        shear_coef = (-shear_ratio[None, None, None, :] * binned).astype(jnp.bfloat16).astype(jnp.float32)
        kappa_map = jnp.einsum('bmcl,mrl->brcm', binned, legendre, precision=highest)
        plus_map = jnp.einsum('bmcl,mrl->brcm', shear_coef, plus_table, precision=highest)
        minus_map = jnp.einsum('bmcl,mrl->brcm', shear_coef, minus_table, precision=highest)
        rotated = jnp.stack([-minus_map[:, :, 1], minus_map[:, :, 0]], axis=2)
        summed = summed + jnp.stack([kappa_map, plus_map, rotated], axis=1)
    return summed
```

```python
import functools

import jax
import jax.numpy as jnp
from jax import lax
from jax.experimental import pallas as pl
from jax.experimental.pallas import tpu as pltpu
from jax.sharding import PartitionSpec as P

TILE = 256


def split(x):
    high = x.astype(jnp.bfloat16)
    low = (x - high.astype(jnp.float32)).astype(jnp.bfloat16)
    return high, low


def maps_kernel(
    first_shell_ref, source_ref, modes_ref, legendre_ref, plus_ref, minus_ref, window_ref, lensing_ref,
    out_ref, left_ref, sums_ref, *, bins, orders, cycles, degrees,
):
    shells = window_ref.shape[0]
    rows = 2 * bins
    sub = lax.broadcasted_iota(jnp.int32, (rows, shells), 0)
    shell_ids = first_shell_ref[0] + lax.broadcasted_iota(jnp.int32, (rows, shells), 1)
    source = jnp.zeros((rows, shells), jnp.int32)
    for b in range(bins):
        source = jnp.where(sub % bins == b, source_ref[b], source)
    efficiency = (
        lensing_ref[...]
        * jnp.maximum(source - shell_ids, 0).astype(jnp.float32)
        / (source + 1).astype(jnp.float32)
    )
    first_part = (sub < bins)[None]
    for m in range(orders):
        real = jnp.broadcast_to(modes_ref[:, m : m + 1, :], (cycles, rows, shells))
        imag = jnp.broadcast_to(modes_ref[:, orders + m : orders + m + 1, :], (cycles, rows, shells))
        left = (jnp.where(first_part, real, imag) * efficiency[None]).reshape(cycles * rows, shells)
        high, low = split(left)
        span = pl.ds(m * cycles * rows, cycles * rows)
        left_ref[span, 0:shells] = high
        left_ref[span, shells : 2 * shells] = low
        left_ref[span, 2 * shells : 3 * shells] = high

    def step(start, sums):
        lanes = pl.ds(start, TILE)
        high, low = split(window_ref[:, lanes])
        product = jnp.dot(
            left_ref[...], jnp.concatenate([high, high, low], 0), preferred_element_type=jnp.float32
        )
        parts = []
        for m in range(orders):
            binned = jnp.zeros((rows, TILE), jnp.float32)
            for r in range(cycles):
                at = (m * cycles + r) * rows
                binned = binned + legendre_ref[m, r : r + 1, lanes] * product[at : at + rows]
            parts.append(binned)
        binned = jnp.concatenate(parts, 0)
        degree = (start + lax.broadcasted_iota(jnp.int32, (rows, TILE), 1)).astype(jnp.float32)
        ratio = jnp.where(
            degree >= 2.0,
            jnp.sqrt((degree + 2.0) * (degree - 1.0) / jnp.maximum(degree * (degree + 1.0), 1.0)),
            0.0,
        )
        ratio = jnp.concatenate([ratio] * orders, 0)
        shear = (-ratio * binned).astype(jnp.bfloat16)
        high, low = split(binned)
        table_high, table_low = split(legendre_ref[:, :, lanes].reshape(orders * cycles, TILE))
        tables = jnp.concatenate(
            [
                table_high,
                table_low,
                plus_ref[:, :, lanes].reshape(orders * cycles, TILE),
                minus_ref[:, :, lanes].reshape(orders * cycles, TILE),
            ],
            0,
        )
        return sums + lax.dot_general(
            jnp.concatenate([high, low, shear], 0),
            tables,
            (((1,), (1,)), ((), ())),
            preferred_element_type=jnp.float32,
        )

    columns = orders * cycles
    sums = jnp.zeros((3 * orders * rows, 4 * columns), jnp.float32)
    if cycles * orders <= 64:
        for start in range(0, degrees, TILE):
            sums = step(start, sums)
        sums_ref[...] = sums
    else:
        sums_ref[...] = sums

        @pl.loop(0, degrees // TILE)
        def _(i):
            sums_ref[...] = step(pl.multiple_of(i * TILE, TILE), sums_ref[...])

    lane = lax.broadcasted_iota(jnp.int32, (rows, columns), 1)

    def own(kind, table):
        total = jnp.zeros((rows, columns), jnp.float32)
        for m in range(orders):
            block = sums_ref[pl.ds((kind * orders + m) * rows, rows), table * columns : (table + 1) * columns]
            total = jnp.where(lane // cycles == m, block, total)
        return total

    out_ref[0] = own(0, 0) + own(0, 1) + own(1, 0)
    out_ref[1] = own(2, 2)
    minus = own(2, 3)
    turned = jnp.concatenate([-minus[bins:], minus[:bins]], 0)
    out_ref[2] = turned


def on_device(
    cycle_modes, cycle_weight, legendre, spin_plus, spin_minus, window, lensing, source_shell
):
    bands = lax.axis_size("band")
    shell_parts = lax.axis_size("shell")
    shells, cycles_here, _, orders_all = cycle_modes.shape
    orders, cycles, degrees = legendre.shape
    bins = source_shell.shape[0]
    own_bins = bins // shell_parts
    weighted = cycle_modes.transpose(1, 2, 3, 0) * cycle_weight[:, None, None, None]
    weighted = weighted.reshape(cycles_here, 2, bands, orders, shells).transpose(2, 0, 1, 3, 4)
    weighted = weighted.reshape(bands, cycles_here, 2 * orders, shells)
    modes = lax.all_to_all(weighted, "band", split_axis=0, concat_axis=0, tiled=True)
    modes = modes.reshape(cycles, 2 * orders, shells)
    first_shell = (lax.axis_index("shell") * shells).astype(jnp.int32).reshape(1)
    smem = pl.BlockSpec(memory_space=pltpu.SMEM)
    vmem = pl.BlockSpec(memory_space=pltpu.VMEM)
    maps = pl.pallas_call(
        functools.partial(maps_kernel, bins=bins, orders=orders, cycles=cycles, degrees=degrees),
        in_specs=[smem, smem] + [vmem] * 6,
        out_specs=vmem,
        out_shape=jax.ShapeDtypeStruct((3, 2 * bins, orders * cycles), jnp.float32),
        scratch_shapes=[
            pltpu.VMEM((orders * cycles * 2 * bins, 3 * shells), jnp.bfloat16),
            pltpu.VMEM((3 * orders * 2 * bins, 4 * orders * cycles), jnp.float32),
        ],
        compiler_params=pltpu.CompilerParams(vmem_limit_bytes=24 * 2**20),
        name="maps",
    )(first_shell, source_shell, modes, legendre, spin_plus, spin_minus, window, lensing.reshape(1, shells))
    maps = maps.reshape(3, 2, shell_parts, own_bins, orders, bands, cycles_here).transpose(2, 5, 3, 0, 6, 1, 4)
    block = own_bins * 3 * cycles_here * 2 * orders
    maps = maps.reshape(shell_parts * bands, block)
    got = lax.all_to_all(maps, ("shell", "band"), split_axis=0, concat_axis=0, tiled=True)
    got = got.reshape(shell_parts, bands, own_bins, 3, cycles_here, 2, orders).sum(0)
    return got.transpose(1, 2, 3, 4, 0, 5).reshape(own_bins, 3, cycles_here, 2, orders_all)


def solution(mesh):
    placed = (
        P(("cosmo", "shell"), "band", None, None),
        P("band"),
        P("band", None, None),
        P("band", None, None),
        P("band", None, None),
        P("shell", None),
        P(("cosmo", "shell")),
        P("cosmo"),
    )
    return jax.shard_map(
        on_device,
        mesh=mesh,
        in_specs=placed,
        out_specs=P(("cosmo", "shell"), None, "band", None, None),
        check_vma=False,
    )
```

```python
import functools

import jax
import jax.numpy as jnp
from jax import lax
from jax.experimental import pallas as pl
from jax.experimental.pallas import tpu as pltpu
from jax.sharding import PartitionSpec as P

TILE = 512
VMEM = pl.BlockSpec(memory_space=pltpu.VMEM)
HBM = pl.BlockSpec(memory_space=pltpu.HBM)
PARAMS = pltpu.CompilerParams(vmem_limit_bytes=28 * 2**20)
KAPPA_HIGH, KAPPA_LOW, PLUS, MINUS = range(4)


def keep(x):
    return pltpu.with_memory_space_constraint(x, pltpu.HBM)


def split(x):
    high = x.astype(jnp.bfloat16)
    low = (x - high.astype(jnp.float32)).astype(jnp.bfloat16)
    return high, low


def iota(shape, axis):
    return lax.broadcasted_iota(jnp.int32, shape, axis)


def pack_kernel(modes_in, weight_in, *out_refs, bands, orders, by_offset):
    *out_refs, blocks_ref, modes_ref, weight_ref, sems = out_refs
    cycles_here, _, _, shells = modes_ref.shape
    copies = [
        pltpu.make_async_copy(modes_in, modes_ref, sems.at[0]),
        pltpu.make_async_copy(weight_in, weight_ref, sems.at[1]),
    ]
    for copy in copies:
        copy.start()
    for copy in copies:
        copy.wait()
    for r in range(cycles_here):
        weight = jnp.broadcast_to(weight_ref[0:1, r : r + 1], (orders, shells))
        for c in range(2):
            for z in range(bands):
                blocks_ref[z, r, c * orders : (c + 1) * orders, :] = (
                    modes_ref[r, c, z * orders : (z + 1) * orders, :] * weight
                )
    if by_offset:
        here = lax.axis_index("band")
        for k in range(bands):
            out_refs[k][...] = blocks_ref[here ^ k]
    else:
        out_refs[0][...] = blocks_ref[...]


def left_of(modes, efficiency, orders, bins):
    cycles, _, shells = modes.shape
    rows = 2 * bins
    first_part = (iota((1, rows, shells), 1) < bins)
    parts = []
    for m in range(orders):
        real = jnp.broadcast_to(modes[:, m : m + 1, :], (cycles, rows, shells))
        imag = jnp.broadcast_to(modes[:, orders + m : orders + m + 1, :], (cycles, rows, shells))
        left = jnp.where(first_part, real, imag) * efficiency[None]
        parts.append(left.reshape(cycles * rows, shells))
    high, low = split(jnp.concatenate(parts, 0))
    return jnp.concatenate([high, low], 1), high


def add_cycles(binned, left, left_high, high, low, legendre_ref, firsts, lanes, orders, rows):
    product = jnp.dot(left, jnp.concatenate([high, high], 0), preferred_element_type=jnp.float32)
    product = product + jnp.dot(left_high, low, preferred_element_type=jnp.float32)
    out = []
    at = 0
    for m in range(orders):
        total = binned[m]
        for first, count in firsts:
            for r in range(count):
                total = total + legendre_ref[m, pl.ds(first + r, 1), lanes] * product[at : at + rows]
                at += rows
        out.append(total)
    return out


def prepare_kernel(
    source_in, lensing_in, legendre_in, plus_in, minus_in, window_in, *refs,
    bins, orders, cycles, cycles_here, degrees, chunk, own,
):
    if own:
        own_ref, *refs = refs
    efficiency_ref, legendre_ref, high_ref, low_ref, tables_ref, binned_ref = refs[:6]
    window_ref, plus_ref, minus_ref, source_ref, lensing_ref, sems, small_sems = refs[6:]
    shells = window_ref.shape[0]
    rows = 2 * bins
    bands = cycles // cycles_here

    def copies(i):
        lanes = pl.ds(i * chunk, chunk)
        return [
            pltpu.make_async_copy(window_in.at[:, lanes], window_ref.at[:, lanes], sems.at[0, i]),
            pltpu.make_async_copy(legendre_in.at[:, :, lanes], legendre_ref.at[:, :, lanes], sems.at[1, i]),
            pltpu.make_async_copy(plus_in.at[:, :, lanes], plus_ref.at[:, :, lanes], sems.at[2, i]),
            pltpu.make_async_copy(minus_in.at[:, :, lanes], minus_ref.at[:, :, lanes], sems.at[3, i]),
        ]

    chunks = degrees // chunk
    small = [
        pltpu.make_async_copy(source_in, source_ref, small_sems.at[0]),
        pltpu.make_async_copy(lensing_in, lensing_ref, small_sems.at[1]),
    ]
    for copy in small:
        copy.start()
    for i in range(chunks):
        for copy in copies(i):
            copy.start()
    for copy in small:
        copy.wait()

    row_bin = iota((rows, shells), 0) % bins
    source = jnp.zeros((rows, shells), jnp.int32)
    for b in range(bins):
        source = jnp.where(row_bin == b, jnp.broadcast_to(source_ref[0:1, b : b + 1], (rows, shells)), source)
    shell_ids = lax.axis_index("shell") * shells + iota((rows, shells), 1)
    efficiency = (
        lensing_ref[...]
        * jnp.maximum(source - shell_ids, 0).astype(jnp.float32)
        / (source + 1).astype(jnp.float32)
    )
    efficiency_ref[...] = efficiency
    if own:
        left, left_high = left_of(own_ref[...], efficiency, orders, bins)
        first = lax.axis_index("band") * cycles_here

    for i in range(chunks):
        lanes = pl.ds(i * chunk, chunk)
        for copy in copies(i):
            copy.wait()
        high, low = split(window_ref[:, lanes])
        high_ref[:, lanes] = high
        low_ref[:, lanes] = low
        for z in range(bands):
            at = z * cycles_here

            def rows_of(ref):
                return jnp.concatenate(
                    [ref[m, :, lanes].astype(jnp.float32)[at : at + cycles_here] for m in range(orders)], 0
                )

            table_high, table_low = split(rows_of(legendre_ref))
            block = orders * cycles_here
            for table, value in (
                (KAPPA_HIGH, table_high),
                (KAPPA_LOW, table_low),
                (PLUS, rows_of(plus_ref).astype(jnp.bfloat16)),
                (MINUS, rows_of(minus_ref).astype(jnp.bfloat16)),
            ):
                tables_ref[pl.ds((z * 4 + table) * block, block), lanes] = value
        if own:
            zero = [jnp.zeros((rows, chunk), jnp.float32)] * orders
            binned = add_cycles(
                zero, left, left_high, high, low, legendre_ref, [(first, cycles_here)], lanes, orders, rows
            )
            binned_ref[:, lanes] = jnp.concatenate(binned, 0)
        else:
            binned_ref[:, lanes] = jnp.zeros((orders * rows, chunk), jnp.float32)


def maps_kernel(
    efficiency_ref, legendre_ref, high_ref, low_ref, tables_ref, binned_ref, *refs,
    bins, orders, cycles_here, by_offset,
):
    *modes_refs, out_ref, left_ref, left_high_ref, sums_ref = refs
    degrees = legendre_ref.shape[2]
    shells = high_ref.shape[0]
    rows = 2 * bins
    bands = legendre_ref.shape[1] // cycles_here
    if by_offset:
        here = lax.axis_index("band")
        firsts = [((here ^ k) * cycles_here, cycles_here) for k in range(1, bands)]
        modes = jnp.concatenate([ref[...] for ref in modes_refs], 0)
    else:
        firsts = [(0, bands * cycles_here)]
        modes = modes_refs[0][...].reshape(bands * cycles_here, 2 * orders, shells)
    left, left_high = left_of(modes, efficiency_ref[...], orders, bins)
    left_ref[...] = left
    left_high_ref[...] = left_high

    def step(start, sums):
        lanes = pl.ds(start, TILE)
        binned = [binned_ref[pl.ds(m * rows, rows), lanes] for m in range(orders)]
        binned = add_cycles(
            binned, left_ref[...], left_high_ref[...], high_ref[:, lanes], low_ref[:, lanes],
            legendre_ref, firsts, lanes, orders, rows,
        )
        binned = jnp.concatenate(binned, 0)
        degree = (start + iota((rows, TILE), 1)).astype(jnp.float32)
        ratio = jnp.where(
            degree >= 2.0,
            jnp.sqrt((degree + 2.0) * (degree - 1.0) / jnp.maximum(degree * (degree + 1.0), 1.0)),
            0.0,
        )
        shear = (-jnp.concatenate([ratio] * orders, 0) * binned).astype(jnp.bfloat16)
        high, low = split(binned)
        return sums + lax.dot_general(
            jnp.concatenate([high, low, shear], 0),
            tables_ref[:, lanes],
            (((1,), (1,)), ((), ())),
            preferred_element_type=jnp.float32,
        )

    block = orders * cycles_here
    sums = jnp.zeros((3 * orders * rows, 4 * bands * block), jnp.float32)
    if by_offset:
        for start in range(0, degrees, TILE):
            sums = step(start, sums)
        sums_ref[...] = sums
    else:
        sums_ref[...] = sums

        @pl.loop(0, degrees // TILE)
        def _(i):
            sums_ref[...] = step(pl.multiple_of(i * TILE, TILE), sums_ref[...])

    width = 8 * block
    lane = iota((rows, width), 1)
    table = lane % (4 * block) // block
    order = lane % block // cycles_here
    first_half = iota((bins, width), 1) < 4 * block
    for pair in range(bands // 2):

        def own(kind):
            total = jnp.zeros((rows, width), jnp.float32)
            for m in range(orders):
                part = sums_ref[pl.ds((kind * orders + m) * rows, rows), pair * width : (pair + 1) * width]
                total = jnp.where(order == m, part, total)
            return total

        kappa = own(0) + jnp.where(table == KAPPA_HIGH, own(1), 0.0)
        value = jnp.where(table < PLUS, kappa, own(2))
        turned = pltpu.roll(value, 4 * block, 1)
        even = jnp.where(first_half, value[:bins], turned[bins:])
        odd = jnp.where(first_half, turned[:bins], value[bins:])
        for b in range(bins):
            out_ref[b * bands + 2 * pair] = even[b : b + 1]
            out_ref[b * bands + 2 * pair + 1] = odd[b : b + 1]


def unpack_kernel(got_ref, out_ref, *, bands, orders, cycles_here):
    width = got_ref.shape[2]
    groups = got_ref.shape[0] // bands
    block = orders * cycles_here
    own_order = iota((orders, width), 1) % block // cycles_here == iota((orders, width), 0)
    columns = []
    for z in range(bands):
        total = got_ref[z]
        for p in range(1, groups):
            total = total + got_ref[p * bands + z]
        columns.append(jnp.where(own_order, jnp.broadcast_to(total, (orders, width)), 0.0))
    values = jnp.concatenate(columns, 0)
    shape = (3 * cycles_here * 2, width)
    row, lane = iota(shape, 0), iota(shape, 1)
    field, cycle, part = row // (2 * cycles_here), row // 2 % cycles_here, row % 2
    lane_part, table = lane // (4 * block), lane // block % 4
    pick = jnp.where(
        field == 0,
        jnp.where((table <= KAPPA_LOW) & (lane_part == part), 1.0, 0.0),
        jnp.where(
            field == 1,
            jnp.where((table == PLUS) & (lane_part == part), 1.0, 0.0),
            jnp.where((table == MINUS) & (lane_part != part), jnp.where(part == 0, -1.0, 1.0), 0.0),
        ),
    )
    pick = jnp.where(lane % cycles_here == cycle, pick, 0.0)
    maps = lax.dot_general(
        pick, values, (((1,), (1,)), ((), ())),
        precision=lax.Precision.HIGHEST, preferred_element_type=jnp.float32,
    )
    for i in range(3 * cycles_here):
        out_ref[i] = maps[2 * i : 2 * i + 2]


def on_device(
    cycle_modes, cycle_weight, legendre, spin_plus, spin_minus, window, lensing, source_shell
):
    bands = lax.axis_size("band")
    shell_parts = lax.axis_size("shell")
    shells, cycles_here, _, orders_all = cycle_modes.shape
    orders, cycles, degrees = legendre.shape
    bins = source_shell.shape[0]
    assert bins == shell_parts and bands % 2 == 0
    by_offset = bands <= 4
    rows = 2 * bins
    columns = 4 * orders * cycles
    chunk = degrees // 4

    def shaped(*shape, dtype=jnp.float32):
        return jax.ShapeDtypeStruct(shape, dtype)

    block_shape = (cycles_here, 2 * orders, shells)
    pack = functools.partial(pack_kernel, bands=bands, orders=orders, by_offset=by_offset)
    operands = keep(cycle_modes.transpose(1, 2, 3, 0)), keep(cycle_weight.reshape(1, cycles_here))
    scratch = [
        pltpu.VMEM((bands, *block_shape), jnp.float32),
        pltpu.VMEM((cycles_here, 2, orders_all, shells), jnp.float32),
        pltpu.VMEM((1, cycles_here), jnp.float32),
        pltpu.SemaphoreType.DMA((2,)),
    ]
    if by_offset:
        own, *sends = pl.pallas_call(
            pack, in_specs=[HBM] * 2, out_specs=[VMEM] * bands, out_shape=[shaped(*block_shape)] * bands,
            scratch_shapes=scratch, compiler_params=PARAMS, name="pack",
        )(*operands)
        modes = [
            lax.ppermute(send, "band", [(z, z ^ k) for z in range(bands)])
            for k, send in enumerate(sends, 1)
        ]
        own = [own]
    else:
        blocks = pl.pallas_call(
            pack, in_specs=[HBM] * 2, out_specs=VMEM, out_shape=shaped(bands, *block_shape),
            scratch_shapes=scratch, compiler_params=PARAMS, name="pack",
        )(*operands)
        modes = [lax.all_to_all(blocks, "band", split_axis=0, concat_axis=0, tiled=True)]
        own = []
    prepared = pl.pallas_call(
        functools.partial(
            prepare_kernel, bins=bins, orders=orders, cycles=cycles, cycles_here=cycles_here,
            degrees=degrees, chunk=chunk, own=by_offset,
        ),
        in_specs=[HBM] * 6 + [VMEM] * len(own),
        out_specs=[VMEM] * 6,
        out_shape=[
            shaped(rows, shells), shaped(orders, cycles, degrees),
            shaped(shells, degrees, dtype=jnp.bfloat16), shaped(shells, degrees, dtype=jnp.bfloat16),
            shaped(columns, degrees, dtype=jnp.bfloat16), shaped(orders * rows, degrees),
        ],
        scratch_shapes=[
            pltpu.VMEM((shells, degrees), jnp.float32),
            pltpu.VMEM((orders, cycles, degrees), jnp.bfloat16),
            pltpu.VMEM((orders, cycles, degrees), jnp.bfloat16),
            pltpu.VMEM((1, bins), jnp.int32),
            pltpu.VMEM((1, shells), jnp.float32),
            pltpu.SemaphoreType.DMA((4, degrees // chunk)),
            pltpu.SemaphoreType.DMA((2,)),
        ],
        compiler_params=PARAMS,
        name="prepare",
    )(
        keep(source_shell.reshape(1, bins)), keep(lensing.reshape(1, shells)), keep(legendre),
        keep(spin_plus), keep(spin_minus), keep(window), *own,
    )
    arriving = orders * (cycles - cycles_here if by_offset else cycles) * rows
    maps = pl.pallas_call(
        functools.partial(maps_kernel, bins=bins, orders=orders, cycles_here=cycles_here, by_offset=by_offset),
        in_specs=[VMEM] * (6 + len(modes)),
        out_specs=VMEM,
        out_shape=shaped(bins * bands, 1, 8 * orders * cycles_here),
        scratch_shapes=[
            pltpu.VMEM((arriving, 2 * shells), jnp.bfloat16),
            pltpu.VMEM((arriving, shells), jnp.bfloat16),
            pltpu.VMEM((3 * orders * rows, columns), jnp.float32),
        ],
        compiler_params=PARAMS,
        name="maps",
    )(*prepared, *modes)
    got = lax.all_to_all(maps, ("shell", "band"), split_axis=0, concat_axis=0, tiled=True)
    out = pl.pallas_call(
        functools.partial(unpack_kernel, bands=bands, orders=orders, cycles_here=cycles_here),
        in_specs=[VMEM],
        out_specs=VMEM,
        out_shape=shaped(3 * cycles_here, 2, orders_all),
        compiler_params=PARAMS,
        name="unpack",
    )(got)
    return out.reshape(1, 3, cycles_here, 2, orders_all)


def solution(mesh):
    placed = (
        P(("cosmo", "shell"), "band", None, None),
        P("band"),
        P("band", None, None),
        P("band", None, None),
        P("band", None, None),
        P("shell", None),
        P(("cosmo", "shell")),
        P("cosmo"),
    )
    return jax.shard_map(
        on_device,
        mesh=mesh,
        in_specs=placed,
        out_specs=P(("cosmo", "shell"), None, "band", None, None),
        check_vma=False,
    )
```

```python
import functools

import jax
import jax.numpy as jnp
from jax import lax
from jax.experimental import pallas as pl
from jax.experimental.pallas import tpu as pltpu
from jax.sharding import PartitionSpec as P

TILE = 512
VMEM = pl.BlockSpec(memory_space=pltpu.VMEM)
HBM = pl.BlockSpec(memory_space=pltpu.HBM)
PARAMS = pltpu.CompilerParams(vmem_limit_bytes=28 * 2**20)
KAPPA_HIGH, KAPPA_LOW, PLUS, MINUS = range(4)


def keep(x):
    return pltpu.with_memory_space_constraint(x, pltpu.HBM)


def split(x):
    high = x.astype(jnp.bfloat16)
    low = (x - high.astype(jnp.float32)).astype(jnp.bfloat16)
    return high, low


def iota(shape, axis):
    return lax.broadcasted_iota(jnp.int32, shape, axis)


def pack_kernel(
    modes_in, weight_in, source_in, lensing_in, *refs, bands, orders, bins, offsets,
):
    *out_refs, efficiency_ref, blocks_ref, modes_ref, weight_ref, source_ref, lensing_ref, sems = refs
    cycles_here, _, _, shells = modes_ref.shape
    pairs = (
        (modes_in, modes_ref), (weight_in, weight_ref), (source_in, source_ref), (lensing_in, lensing_ref),
    )
    copies = [pltpu.make_async_copy(*pair, sems.at[i]) for i, pair in enumerate(pairs)]
    for copy in copies:
        copy.start()
    for copy in copies:
        copy.wait()
    for r in range(cycles_here):
        weight = jnp.broadcast_to(weight_ref[0:1, r : r + 1], (orders, shells))
        for c in range(2):
            for z in range(bands):
                blocks_ref[z, r, c * orders : (c + 1) * orders, :] = (
                    modes_ref[r, c, z * orders : (z + 1) * orders, :] * weight
                )
    if offsets:
        here = lax.axis_index("band")
        for k, out_ref in zip((0, *offsets), out_refs):
            out_ref[...] = blocks_ref[here ^ k]
    else:
        out_refs[0][...] = blocks_ref[...]
    rows = 2 * bins
    row_bin = iota((rows, shells), 0) % bins
    source = jnp.zeros((rows, shells), jnp.int32)
    for b in range(bins):
        source = jnp.where(row_bin == b, jnp.broadcast_to(source_ref[0:1, b : b + 1], (rows, shells)), source)
    shell_ids = lax.axis_index("shell") * shells + iota((rows, shells), 1)
    efficiency_ref[...] = (
        lensing_ref[...]
        * jnp.maximum(source - shell_ids, 0).astype(jnp.float32)
        / (source + 1).astype(jnp.float32)
    )


def left_of(modes, efficiency, orders, bins):
    cycles, _, shells = modes.shape
    rows = 2 * bins
    first_part = (iota((1, rows, shells), 1) < bins)
    parts = []
    for m in range(orders):
        real = jnp.broadcast_to(modes[:, m : m + 1, :], (cycles, rows, shells))
        imag = jnp.broadcast_to(modes[:, orders + m : orders + m + 1, :], (cycles, rows, shells))
        left = jnp.where(first_part, real, imag) * efficiency[None]
        parts.append(left.reshape(cycles * rows, shells))
    high, low = split(jnp.concatenate(parts, 0))
    return jnp.concatenate([high, low], 1), high


def add_cycles(binned, left, left_high, high, low, legendre_ref, firsts, lanes, orders, rows):
    product = jnp.dot(left, jnp.concatenate([high, high], 0), preferred_element_type=jnp.float32)
    product = product + jnp.dot(left_high, low, preferred_element_type=jnp.float32)
    out = []
    at = 0
    for m in range(orders):
        total = binned[m]
        for first, count in firsts:
            for r in range(count):
                total = total + legendre_ref[m, pl.ds(first + r, 1), lanes] * product[at : at + rows]
                at += rows
        out.append(total)
    return out


def prepare_kernel(window_ref, legendre_ref, high_ref, low_ref, table_high_ref, table_low_ref):
    high_ref[...], low_ref[...] = split(window_ref[...])
    table_high_ref[...], table_low_ref[...] = split(legendre_ref[...])


def each_tile(degrees, unroll, step):
    if unroll:
        for start in range(0, degrees, TILE):
            step(start)
    else:
        pl.loop(0, degrees // TILE)(lambda i: step(pl.multiple_of(i * TILE, TILE)))


def gather_left(modes_refs, efficiency_ref, left_ref, left_high_ref, orders, cycles_here, offsets):
    if offsets:
        here = lax.axis_index("band")
        firsts = [((here ^ k) * cycles_here, cycles_here) for k in offsets]
        modes = jnp.concatenate([ref[...] for ref in modes_refs], 0)
    else:
        modes = modes_refs[0][...]
        modes = modes.reshape(-1, *modes.shape[2:])
        firsts = [(0, modes.shape[0])]
    left_ref[...], left_high_ref[...] = left_of(
        modes, efficiency_ref[...], orders, efficiency_ref.shape[0] // 2
    )
    return firsts


def first_kernel(
    efficiency_ref, legendre_ref, high_ref, low_ref, *refs, orders, cycles_here, offsets,
):
    *modes_refs, binned_ref, left_ref, left_high_ref = refs
    rows = efficiency_ref.shape[0]
    firsts = gather_left(modes_refs, efficiency_ref, left_ref, left_high_ref, orders, cycles_here, offsets)

    def step(start):
        lanes = pl.ds(start, TILE)
        binned = add_cycles(
            [jnp.zeros((rows, TILE), jnp.float32)] * orders, left_ref[...], left_high_ref[...],
            high_ref[:, lanes], low_ref[:, lanes], legendre_ref, firsts, lanes, orders, rows,
        )
        for m in range(orders):
            binned_ref[pl.ds(m * rows, rows), lanes] = binned[m]

    each_tile(legendre_ref.shape[2], True, step)


def maps_kernel(
    efficiency_ref, legendre_ref, high_ref, low_ref, table_high_ref, table_low_ref, plus_ref, minus_ref, *refs,
    bands, orders, cycles_here, offsets,
):
    if offsets:
        binned_ref, *refs = refs
    *modes_refs, out_ref, left_ref, left_high_ref, sums_ref = refs
    cycles = legendre_ref.shape[1]
    rows = efficiency_ref.shape[0]
    bins = rows // 2
    columns = orders * cycles
    firsts = gather_left(modes_refs, efficiency_ref, left_ref, left_high_ref, orders, cycles_here, offsets)
    sums_ref[...] = jnp.zeros(sums_ref.shape, jnp.float32)

    def step(start):
        lanes = pl.ds(start, TILE)
        if offsets:
            binned = [binned_ref[pl.ds(m * rows, rows), lanes] for m in range(orders)]
        else:
            binned = [jnp.zeros((rows, TILE), jnp.float32)] * orders
        binned = add_cycles(
            binned, left_ref[...], left_high_ref[...], high_ref[:, lanes], low_ref[:, lanes],
            legendre_ref, firsts, lanes, orders, rows,
        )
        binned = jnp.concatenate(binned, 0)
        degree = (start + iota((rows, TILE), 1)).astype(jnp.float32)
        ratio = jnp.where(
            degree >= 2.0,
            jnp.sqrt((degree + 2.0) * (degree - 1.0) / jnp.maximum(degree * (degree + 1.0), 1.0)),
            0.0,
        )
        shear = (-jnp.concatenate([ratio] * orders, 0) * binned).astype(jnp.bfloat16)
        high, low = split(binned)
        tables = [
            ref[:, :, lanes].reshape(columns, TILE)
            for ref in (table_high_ref, table_low_ref, plus_ref, minus_ref)
        ]
        sums_ref[...] += lax.dot_general(
            jnp.concatenate([high, low, shear], 0), jnp.concatenate(tables, 0),
            (((1,), (1,)), ((), ())),
            preferred_element_type=jnp.float32,
        )

    each_tile(legendre_ref.shape[2], bool(offsets), step)

    lane = iota((rows, 4 * columns), 1)
    table = lane // columns
    order = lane % columns // cycles

    def own(kind):
        total = jnp.zeros((rows, 4 * columns), jnp.float32)
        for m in range(orders):
            total = jnp.where(order == m, sums_ref[pl.ds((kind * orders + m) * rows, rows), :], total)
        return total

    kappa = own(0) + jnp.where(table == KAPPA_HIGH, own(1), 0.0)
    value = jnp.where(table < PLUS, kappa, own(2))
    for b in range(bins):
        for z in range(bands):
            for c in range(2):
                out_ref[b * bands + z, c : c + 1, :] = value[c * bins + b : c * bins + b + 1]


def unpack_kernel(got_ref, out_ref, *, bands, orders, cycles_here):
    width = got_ref.shape[2]
    groups = got_ref.shape[0] // bands
    cycles = bands * cycles_here
    columns = orders * cycles
    own_order = iota((orders, width), 1) % columns // cycles == iota((orders, width), 0)
    shape = (3 * cycles_here * 2, width)
    row, lane = iota(shape, 0), iota(shape, 1)
    field, cycle, part = row // (2 * cycles_here), row // 2 % cycles_here, row % 2
    table = lane // columns
    here = lane % cycles == lax.axis_index("band") * cycles_here + cycle
    total = [got_ref[z] for z in range(bands)]
    for p in range(1, groups):
        total = [total[z] + got_ref[p * bands + z] for z in range(bands)]
    maps = jnp.zeros((3 * cycles_here * 2, bands * orders), jnp.float32)
    for c in range(2):
        values = jnp.concatenate(
            [
                jnp.where(own_order, jnp.broadcast_to(total[z][c : c + 1], (orders, width)), 0.0)
                for z in range(bands)
            ],
            0,
        )
        same = jnp.where(part == c, 1.0, 0.0)
        other = jnp.where(part == c, 0.0, 1.0 if c == 0 else -1.0)
        pick = jnp.where(
            field == 0,
            jnp.where(table <= KAPPA_LOW, same, 0.0),
            jnp.where(field == 1, jnp.where(table == PLUS, same, 0.0), jnp.where(table == MINUS, other, 0.0)),
        )
        maps = maps + lax.dot_general(
            jnp.where(here, pick, 0.0), values, (((1,), (1,)), ((), ())),
            precision=lax.Precision.HIGHEST, preferred_element_type=jnp.float32,
        )
    for i in range(3 * cycles_here):
        out_ref[i] = maps[2 * i : 2 * i + 2]


def on_device(
    cycle_modes, cycle_weight, legendre, spin_plus, spin_minus, window, lensing, source_shell
):
    bands = lax.axis_size("band")
    shell_parts = lax.axis_size("shell")
    shells, cycles_here, _, orders_all = cycle_modes.shape
    orders, cycles, degrees = legendre.shape
    bins = source_shell.shape[0]
    assert bins == shell_parts
    offsets = (2, 3, 1) if bands == 4 else ()
    rows = 2 * bins
    columns = 4 * orders * cycles

    def shaped(*shape, dtype=jnp.float32):
        return jax.ShapeDtypeStruct(shape, dtype)

    def left_scratch(blocks):
        return [
            pltpu.VMEM((orders * blocks * cycles_here * rows, 2 * shells), jnp.bfloat16),
            pltpu.VMEM((orders * blocks * cycles_here * rows, shells), jnp.bfloat16),
        ]

    block_shape = (cycles_here, 2 * orders, shells)
    out_shape = [shaped(*block_shape)] * bands if offsets else [shaped(bands, *block_shape)]
    out_shape = [*out_shape, shaped(rows, shells)]
    *blocks, efficiency = pl.pallas_call(
        functools.partial(pack_kernel, bands=bands, orders=orders, bins=bins, offsets=offsets),
        in_specs=[HBM] * 4,
        out_specs=[VMEM] * len(out_shape),
        out_shape=out_shape,
        scratch_shapes=[
            pltpu.VMEM((bands, *block_shape), jnp.float32),
            pltpu.VMEM((cycles_here, 2, orders_all, shells), jnp.float32),
            pltpu.VMEM((1, cycles_here), jnp.float32),
            pltpu.VMEM((1, bins), jnp.int32),
            pltpu.VMEM((1, shells), jnp.float32),
            pltpu.SemaphoreType.DMA((4,)),
        ],
        compiler_params=PARAMS,
        cost_estimate=pl.CostEstimate(flops=10**10, bytes_accessed=2**17, transcendentals=0),
        name="pack",
    )(
        keep(cycle_modes.transpose(1, 2, 3, 0)), keep(cycle_weight.reshape(1, cycles_here)),
        keep(source_shell.reshape(1, bins)), keep(lensing.reshape(1, shells)),
    )
    if offsets:
        own, *sends = blocks
        got = [
            lax.ppermute(send, "band", [(z, z ^ k) for z in range(bands)])
            for k, send in zip(offsets, sends)
        ]
    else:
        got = [lax.all_to_all(blocks[0], "band", split_axis=0, concat_axis=0, tiled=True)]
    half = jnp.bfloat16
    high, low, table_high, table_low = pl.pallas_call(
        prepare_kernel,
        in_specs=[VMEM] * 2,
        out_specs=[VMEM] * 4,
        out_shape=[shaped(shells, degrees, dtype=half)] * 2 + [shaped(orders, cycles, degrees, dtype=half)] * 2,
        compiler_params=PARAMS,
        name="prepare",
    )(window, legendre)
    operands = [efficiency, legendre, high, low, table_high, table_low, spin_plus, spin_minus]
    last = got
    if offsets:
        last = got[1:]
        operands.append(
            pl.pallas_call(
                functools.partial(
                    first_kernel, orders=orders, cycles_here=cycles_here, offsets=(0, offsets[0])
                ),
                in_specs=[VMEM] * 6,
                out_specs=VMEM,
                out_shape=shaped(orders * rows, degrees),
                scratch_shapes=left_scratch(2),
                compiler_params=PARAMS,
                name="first",
            )(efficiency, legendre, high, low, own, got[0])
        )
    operands += last
    maps = pl.pallas_call(
        functools.partial(
            maps_kernel, bands=bands, orders=orders, cycles_here=cycles_here, offsets=offsets[1:]
        ),
        in_specs=[VMEM] * len(operands),
        out_specs=VMEM,
        out_shape=shaped(bins * bands, 2, columns),
        scratch_shapes=[
            *left_scratch(len(last) if offsets else bands),
            pltpu.VMEM((3 * orders * rows, columns), jnp.float32),
        ],
        compiler_params=PARAMS,
        name="maps",
    )(*operands)
    got = lax.all_to_all(maps, ("shell", "band"), split_axis=0, concat_axis=0, tiled=True)
    out = pl.pallas_call(
        functools.partial(unpack_kernel, bands=bands, orders=orders, cycles_here=cycles_here),
        in_specs=[VMEM],
        out_specs=VMEM,
        out_shape=shaped(3 * cycles_here, 2, orders_all),
        compiler_params=PARAMS,
        name="unpack",
    )(got)
    return out.reshape(1, 3, cycles_here, 2, orders_all)


def solution(mesh):
    placed = (
        P(("cosmo", "shell"), "band", None, None),
        P("band"),
        P("band", None, None),
        P("band", None, None),
        P("band", None, None),
        P("shell", None),
        P(("cosmo", "shell")),
        P("cosmo"),
    )
    return jax.shard_map(
        on_device,
        mesh=mesh,
        in_specs=placed,
        out_specs=P(("cosmo", "shell"), None, "band", None, None),
        check_vma=False,
    )
```

```python
import functools

import jax
import jax.numpy as jnp
from jax import lax
from jax.experimental import pallas as pl
from jax.experimental.pallas import tpu as pltpu
from jax.sharding import PartitionSpec as P

TILE = 256
LANES = 128
VMEM = pl.BlockSpec(memory_space=pltpu.VMEM)
HBM = pl.BlockSpec(memory_space=pltpu.HBM)
PARAMS = pltpu.CompilerParams(vmem_limit_bytes=28 * 2**20)
KAPPA_HIGH, KAPPA_LOW, PLUS, MINUS = range(4)


def keep(x):
    return pltpu.with_memory_space_constraint(x, pltpu.HBM)


def split(x):
    high = x.astype(jnp.bfloat16)
    low = (x - high.astype(jnp.float32)).astype(jnp.bfloat16)
    return high, low


def iota(shape, axis):
    return lax.broadcasted_iota(jnp.int32, shape, axis)


def load_kernel(*refs):
    count = len(refs) // 2
    copies = [pltpu.make_async_copy(refs[i], refs[count + i], refs[-1].at[i]) for i in range(count)]
    for copy in copies:
        copy.start()
    for copy in copies:
        copy.wait()


def pack_kernel(modes_ref, weight_ref, source_ref, lensing_ref, *refs, bands, orders, bins, offsets):
    *out_refs, efficiency_ref, blocks_ref = refs
    cycles_here, _, _, shells = modes_ref.shape
    for r in range(cycles_here):
        weight = jnp.broadcast_to(weight_ref[0:1, r : r + 1], (orders, shells))
        for c in range(2):
            for z in range(bands):
                blocks_ref[z, r, c * orders : (c + 1) * orders, :] = (
                    modes_ref[r, c, z * orders : (z + 1) * orders, :] * weight
                )
    if offsets:
        here = lax.axis_index("band")
        for k, out_ref in zip((0, *offsets), out_refs):
            out_ref[...] = blocks_ref[here ^ k]
    else:
        out_refs[0][...] = blocks_ref[...]
    rows = 2 * bins
    row_bin = iota((rows, shells), 0) % bins
    source = jnp.zeros((rows, shells), jnp.int32)
    for b in range(bins):
        source = jnp.where(row_bin == b, jnp.broadcast_to(source_ref[0:1, b : b + 1], (rows, shells)), source)
    shell_ids = lax.axis_index("shell") * shells + iota((rows, shells), 1)
    efficiency_ref[...] = (
        lensing_ref[...]
        * jnp.maximum(source - shell_ids, 0).astype(jnp.float32)
        / (source + 1).astype(jnp.float32)
    )


def left_of(modes, efficiency, orders, bins):
    cycles, _, shells = modes.shape
    rows = 2 * bins
    first_part = (iota((1, rows, shells), 1) < bins)
    parts = []
    for m in range(orders):
        real = jnp.broadcast_to(modes[:, m : m + 1, :], (cycles, rows, shells))
        imag = jnp.broadcast_to(modes[:, orders + m : orders + m + 1, :], (cycles, rows, shells))
        left = jnp.where(first_part, real, imag) * efficiency[None]
        parts.append(left.reshape(cycles * rows, shells))
    high, low = split(jnp.concatenate(parts, 0))
    return jnp.concatenate([high, low], 1), high


def add_cycles(binned, left, left_high, high, low, legendre_ref, firsts, lanes, orders, rows):
    product = jnp.dot(left, jnp.concatenate([high, high], 0), preferred_element_type=jnp.float32)
    product = product + jnp.dot(left_high, low, preferred_element_type=jnp.float32)
    out = []
    at = 0
    for m in range(orders):
        total = binned[m]
        for first, count in firsts:
            for r in range(count):
                total = total + legendre_ref[m, pl.ds(first + r, 1), lanes] * product[at : at + rows]
                at += rows
        out.append(total)
    return out


def each_tile(degrees, unroll, step):
    if unroll:
        for start in range(0, degrees, TILE):
            step(start)
    else:
        pl.loop(0, degrees // TILE)(lambda i: step(pl.multiple_of(i * TILE, TILE)))


def gather_left(modes_refs, efficiency_ref, left_ref, left_high_ref, orders, cycles_here, offsets):
    if offsets:
        here = lax.axis_index("band")
        firsts = [((here ^ k) * cycles_here, cycles_here) for k in offsets]
        modes = jnp.concatenate([ref[...] for ref in modes_refs], 0)
    else:
        modes = modes_refs[0][...]
        modes = modes.reshape(-1, *modes.shape[2:])
        firsts = [(0, modes.shape[0])]
    left_ref[...], left_high_ref[...] = left_of(
        modes, efficiency_ref[...], orders, efficiency_ref.shape[0] // 2
    )
    return firsts


def prepare_kernel(window_ref, legendre_ref, plus_ref, minus_ref, *refs, orders, cycles_here):
    if len(refs) > 4:
        efficiency_ref, own_ref, *refs, binned_ref, left_ref, left_high_ref = refs
        rows = efficiency_ref.shape[0]
        firsts = gather_left([own_ref], efficiency_ref, left_ref, left_high_ref, orders, cycles_here, (0,))
        own = True
    else:
        own = False
    high_ref, low_ref, table_high_ref, table_low_ref = refs

    def step(start):
        lanes = pl.ds(start, TILE)
        high, low = split(window_ref[:, lanes])
        high_ref[:, lanes], low_ref[:, lanes] = high, low
        table_high_ref[:, :, lanes], table_low_ref[:, :, lanes] = split(legendre_ref[:, :, lanes])
        if own:
            binned = add_cycles(
                [jnp.zeros((rows, TILE), jnp.float32)] * orders, left_ref[...], left_high_ref[...],
                high, low, legendre_ref, firsts, lanes, orders, rows,
            )
            for m in range(orders):
                binned_ref[pl.ds(m * rows, rows), lanes] = binned[m]

    each_tile(legendre_ref.shape[2], own, step)


def more_kernel(
    efficiency_ref, legendre_ref, high_ref, low_ref, binned_in, modes_ref, binned_ref, left_ref, left_high_ref,
    *, orders, cycles_here, offset,
):
    rows = efficiency_ref.shape[0]
    firsts = gather_left([modes_ref], efficiency_ref, left_ref, left_high_ref, orders, cycles_here, (offset,))

    def step(start):
        lanes = pl.ds(start, TILE)
        binned = add_cycles(
            [binned_in[pl.ds(m * rows, rows), lanes] for m in range(orders)], left_ref[...], left_high_ref[...],
            high_ref[:, lanes], low_ref[:, lanes], legendre_ref, firsts, lanes, orders, rows,
        )
        for m in range(orders):
            binned_ref[pl.ds(m * rows, rows), lanes] = binned[m]

    each_tile(legendre_ref.shape[2], True, step)


def maps_kernel(
    efficiency_ref, legendre_ref, high_ref, low_ref, table_high_ref, table_low_ref, plus_ref, minus_ref, *refs,
    bands, orders, cycles_here, offsets,
):
    if offsets:
        binned_ref, *refs = refs
    *modes_refs, out_ref, left_ref, left_high_ref, sums_ref = refs
    cycles = legendre_ref.shape[1]
    rows = efficiency_ref.shape[0]
    bins = rows // 2
    columns = orders * cycles
    firsts = gather_left(modes_refs, efficiency_ref, left_ref, left_high_ref, orders, cycles_here, offsets)
    sums_ref[...] = jnp.zeros(sums_ref.shape, jnp.float32)

    def step(start):
        lanes = pl.ds(start, TILE)
        if offsets:
            binned = [binned_ref[pl.ds(m * rows, rows), lanes] for m in range(orders)]
        else:
            binned = [jnp.zeros((rows, TILE), jnp.float32)] * orders
        binned = add_cycles(
            binned, left_ref[...], left_high_ref[...], high_ref[:, lanes], low_ref[:, lanes],
            legendre_ref, firsts, lanes, orders, rows,
        )
        binned = jnp.concatenate(binned, 0)
        degree = (start + iota((rows, TILE), 1)).astype(jnp.float32)
        ratio = jnp.where(
            degree >= 2.0,
            jnp.sqrt((degree + 2.0) * (degree - 1.0) / jnp.maximum(degree * (degree + 1.0), 1.0)),
            0.0,
        )
        shear = (-jnp.concatenate([ratio] * orders, 0) * binned).astype(jnp.bfloat16)
        high, low = split(binned)
        tables = [
            ref[:, :, lanes].reshape(columns, TILE)
            for ref in (table_high_ref, table_low_ref, plus_ref, minus_ref)
        ]
        sums_ref[...] += lax.dot_general(
            jnp.concatenate([high, low, shear], 0), jnp.concatenate(tables, 0),
            (((1,), (1,)), ((), ())),
            preferred_element_type=jnp.float32,
        )

    each_tile(legendre_ref.shape[2], bool(offsets), step)

    lane = iota((rows, 4 * columns), 1)
    table = lane // columns
    order = lane % columns // cycles

    def own(kind):
        total = jnp.zeros((rows, 4 * columns), jnp.float32)
        for m in range(orders):
            total = jnp.where(order == m, sums_ref[pl.ds((kind * orders + m) * rows, rows), :], total)
        return total

    kappa = own(0) + jnp.where(table == KAPPA_HIGH, own(1), 0.0)
    value = jnp.where(table < PLUS, kappa, own(2))
    count = 4 * columns // LANES
    slot = iota((rows, LANES), 1) % cycles // cycles_here
    shifted = {}
    for z in range(bands):
        halves = []
        for c in range(2):
            half = jnp.zeros((rows, LANES), jnp.float32)
            for v in range(count):
                at = c * count + v
                shift = (at - z) * cycles_here % LANES
                if (v, shift) not in shifted:
                    part = value[:, v * LANES : (v + 1) * LANES]
                    shifted[v, shift] = pltpu.roll(part, shift, 1) if shift else part
                half = jnp.where(slot == at, shifted[v, shift], half)
            halves.append(half)
        row = jnp.where(slot[:bins] < count, halves[0][:bins], halves[1][bins:])
        for b in range(bins):
            out_ref[b * bands + z] = row[b : b + 1]


def unpack_kernel(got_ref, out_ref, *, bands, orders, cycles_here):
    groups = got_ref.shape[0] // bands
    cycles = bands * cycles_here
    columns = orders * cycles
    count = 4 * columns // LANES

    def origin(lane):
        slot = lane % cycles // cycles_here
        source = slot % count * LANES + lane // cycles * cycles
        return slot // count, source // columns, source % columns // cycles

    shape = (orders, LANES)
    own_order = origin(iota(shape, 1))[2] == iota(shape, 0)
    values = []
    for z in range(bands):
        total = got_ref[z]
        for p in range(1, groups):
            total = total + got_ref[p * bands + z]
        values.append(jnp.where(own_order, jnp.broadcast_to(total, shape), 0.0))
    shape = (3 * cycles_here * 2, LANES)
    row, lane = iota(shape, 0), iota(shape, 1)
    field, cycle, part = row // (2 * cycles_here), row // 2 % cycles_here, row % 2
    lane_part, table, _ = origin(lane)
    same = jnp.where(lane_part == part, 1.0, 0.0)
    other = jnp.where(lane_part == part, 0.0, jnp.where(part == 0, -1.0, 1.0))
    pick = jnp.where(
        field == 0,
        jnp.where(table <= KAPPA_LOW, same, 0.0),
        jnp.where(field == 1, jnp.where(table == PLUS, same, 0.0), jnp.where(table == MINUS, other, 0.0)),
    )
    maps = lax.dot_general(
        jnp.where(lane % cycles_here == cycle, pick, 0.0), jnp.concatenate(values, 0), (((1,), (1,)), ((), ())),
        precision=lax.Precision.HIGHEST, preferred_element_type=jnp.float32,
    )
    for i in range(3 * cycles_here):
        out_ref[i] = maps[2 * i : 2 * i + 2]


def on_device(
    cycle_modes, cycle_weight, legendre, spin_plus, spin_minus, window, lensing, source_shell
):
    bands = lax.axis_size("band")
    shell_parts = lax.axis_size("shell")
    shells, cycles_here, _, orders_all = cycle_modes.shape
    orders, cycles, degrees = legendre.shape
    bins = source_shell.shape[0]
    assert bins == shell_parts and 8 * orders * cycles_here == LANES
    offsets = (2, 3, 1) if bands == 4 else ()
    rows = 2 * bins
    columns = 4 * orders * cycles

    def shaped(*shape, dtype=jnp.float32):
        return jax.ShapeDtypeStruct(shape, dtype)

    def left_scratch(blocks):
        return [
            pltpu.VMEM((orders * blocks * cycles_here * rows, 2 * shells), jnp.bfloat16),
            pltpu.VMEM((orders * blocks * cycles_here * rows, shells), jnp.bfloat16),
        ]

    block_shape = (cycles_here, 2 * orders, shells)
    out_shape = [shaped(*block_shape)] * bands if offsets else [shaped(bands, *block_shape)]
    out_shape = [*out_shape, shaped(rows, shells)]
    sources = (
        cycle_modes.transpose(1, 2, 3, 0), cycle_weight.reshape(1, cycles_here),
        source_shell.reshape(1, bins), lensing.reshape(1, shells),
    )
    sources = pl.pallas_call(
        load_kernel,
        in_specs=[HBM] * 4,
        out_specs=[VMEM] * 4,
        out_shape=[shaped(*x.shape, dtype=x.dtype) for x in sources],
        scratch_shapes=[pltpu.SemaphoreType.DMA((4,))],
        compiler_params=PARAMS,
        name="load",
    )(*map(keep, sources))
    *blocks, efficiency = pl.pallas_call(
        functools.partial(pack_kernel, bands=bands, orders=orders, bins=bins, offsets=offsets),
        in_specs=[VMEM] * 4,
        out_specs=[VMEM] * len(out_shape),
        out_shape=out_shape,
        scratch_shapes=[pltpu.VMEM((bands, *block_shape), jnp.float32)],
        compiler_params=PARAMS,
        cost_estimate=pl.CostEstimate(flops=10**10, bytes_accessed=2**17, transcendentals=0),
        name="pack",
    )(*sources)
    if offsets:
        own, *sends = blocks
        got = [
            lax.ppermute(send, "band", [(z, z ^ k) for z in range(bands)])
            for k, send in zip(offsets, sends)
        ]
    else:
        got = [lax.all_to_all(blocks[0], "band", split_axis=0, concat_axis=0, tiled=True)]
    half = jnp.bfloat16
    tables = [shaped(shells, degrees, dtype=half)] * 2 + [shaped(orders, cycles, degrees, dtype=half)] * 2
    binned_shape = shaped(orders * rows, degrees)
    arguments = [window, legendre, spin_plus, spin_minus]
    if offsets:
        tables.append(binned_shape)
        arguments += [efficiency, own]
    high, low, table_high, table_low, *binned = pl.pallas_call(
        functools.partial(prepare_kernel, orders=orders, cycles_here=cycles_here),
        in_specs=[VMEM] * len(arguments),
        out_specs=[VMEM] * len(tables),
        out_shape=tables,
        scratch_shapes=left_scratch(1) if offsets else [],
        compiler_params=PARAMS,
        name="prepare",
    )(*arguments)
    for k, block in zip(offsets[:-1], got):
        binned = [
            pl.pallas_call(
                functools.partial(more_kernel, orders=orders, cycles_here=cycles_here, offset=k),
                in_specs=[VMEM] * 6,
                out_specs=VMEM,
                out_shape=binned_shape,
                scratch_shapes=left_scratch(1),
                compiler_params=PARAMS,
                name="more",
            )(efficiency, legendre, high, low, *binned, block)
        ]
    last = got[-1:]
    operands = [efficiency, legendre, high, low, table_high, table_low, spin_plus, spin_minus, *binned, *last]
    maps = pl.pallas_call(
        functools.partial(
            maps_kernel, bands=bands, orders=orders, cycles_here=cycles_here, offsets=offsets[-1:]
        ),
        in_specs=[VMEM] * len(operands),
        out_specs=VMEM,
        out_shape=shaped(bins * bands, 1, LANES),
        scratch_shapes=[
            *left_scratch(len(last) if offsets else bands),
            pltpu.VMEM((3 * orders * rows, columns), jnp.float32),
        ],
        compiler_params=PARAMS,
        name="maps",
    )(*operands)
    got = lax.all_to_all(maps, ("shell", "band"), split_axis=0, concat_axis=0, tiled=True)
    out = pl.pallas_call(
        functools.partial(unpack_kernel, bands=bands, orders=orders, cycles_here=cycles_here),
        in_specs=[VMEM],
        out_specs=VMEM,
        out_shape=shaped(3 * cycles_here, 2, orders_all),
        compiler_params=PARAMS,
        name="unpack",
    )(got)
    return out.reshape(1, 3, cycles_here, 2, orders_all)


def solution(mesh):
    placed = (
        P(("cosmo", "shell"), "band", None, None),
        P("band"),
        P("band", None, None),
        P("band", None, None),
        P("band", None, None),
        P("shell", None),
        P(("cosmo", "shell")),
        P("cosmo"),
    )
    return jax.shard_map(
        on_device,
        mesh=mesh,
        in_specs=placed,
        out_specs=P(("cosmo", "shell"), None, "band", None, None),
        check_vma=False,
    )
```

```python
import functools

import jax
import jax.numpy as jnp
from jax import lax
from jax.experimental import pallas as pl
from jax.experimental.pallas import tpu as pltpu
from jax.sharding import PartitionSpec as P

TILE = 256
GROUP = 16
LANES = 128
VMEM = pl.BlockSpec(memory_space=pltpu.VMEM)
HBM = pl.BlockSpec(memory_space=pltpu.HBM)
PARAMS = pltpu.CompilerParams(vmem_limit_bytes=28 * 2**20)
KAPPA_HIGH, KAPPA_LOW, PLUS, MINUS = range(4)


def keep(x):
    return pltpu.with_memory_space_constraint(x, pltpu.HBM)


def split(x):
    high = x.astype(jnp.bfloat16)
    low = (x - high.astype(jnp.float32)).astype(jnp.bfloat16)
    return high, low


def iota(shape, axis):
    return lax.broadcasted_iota(jnp.int32, shape, axis)


def load_kernel(*refs):
    count = len(refs) // 2
    copies = [pltpu.make_async_copy(refs[i], refs[count + i], refs[-1].at[i]) for i in range(count)]
    for copy in copies:
        copy.start()
    for copy in copies:
        copy.wait()


def pack_kernel(modes_ref, weight_ref, source_ref, lensing_ref, *refs, bands, orders, bins, offsets):
    *out_refs, efficiency_ref, blocks_ref = refs
    cycles_here, _, _, shells = modes_ref.shape
    for r in range(cycles_here):
        weight = jnp.broadcast_to(weight_ref[0:1, r : r + 1], (orders, shells))
        for c in range(2):
            for z in range(bands):
                blocks_ref[z, r, c * orders : (c + 1) * orders, :] = (
                    modes_ref[r, c, z * orders : (z + 1) * orders, :] * weight
                )
    if offsets:
        here = lax.axis_index("band")
        for k, out_ref in zip((0, *offsets), out_refs):
            out_ref[...] = blocks_ref[here ^ k]
    else:
        out_refs[0][...] = blocks_ref[...]
    rows = 2 * bins
    row_bin = iota((rows, shells), 0) % bins
    source = jnp.zeros((rows, shells), jnp.int32)
    for b in range(bins):
        source = jnp.where(row_bin == b, jnp.broadcast_to(source_ref[0:1, b : b + 1], (rows, shells)), source)
    shell_ids = lax.axis_index("shell") * shells + iota((rows, shells), 1)
    efficiency_ref[...] = (
        lensing_ref[...]
        * jnp.maximum(source - shell_ids, 0).astype(jnp.float32)
        / (source + 1).astype(jnp.float32)
    )


def left_of(modes, efficiency, orders, bins):
    cycles, _, shells = modes.shape
    rows = 2 * bins
    first_part = (iota((1, rows, shells), 1) < bins)
    parts = []
    for m in range(orders):
        real = jnp.broadcast_to(modes[:, m : m + 1, :], (cycles, rows, shells))
        imag = jnp.broadcast_to(modes[:, orders + m : orders + m + 1, :], (cycles, rows, shells))
        left = jnp.where(first_part, real, imag) * efficiency[None]
        parts.append(left.reshape(cycles * rows, shells))
    high, low = split(jnp.concatenate(parts, 0))
    return jnp.concatenate([high, low], 1), high


def multiply(left, left_high, high, low):
    product = jnp.dot(left, jnp.concatenate([high, high], 0), preferred_element_type=jnp.float32)
    return product + jnp.dot(left_high, low, preferred_element_type=jnp.float32)


def add_cycles(binned, product, legendre_ref, firsts, lanes, orders, rows):
    out = []
    at = 0
    for m in range(orders):
        total = binned[m]
        for first, count in firsts:
            for r in range(count):
                total = total + legendre_ref[m, pl.ds(first + r, 1), lanes] * product[at : at + rows]
                at += rows
        out.append(total)
    return out


def each_tile(degrees, unroll, step, size=TILE):
    if unroll:
        for start in range(0, degrees, size):
            step(start)
    else:
        pl.loop(0, degrees // size)(lambda i: step(pl.multiple_of(i * size, size)))


def gather_left(modes_refs, efficiency_ref, left_ref, left_high_ref, orders, cycles_here, offsets):
    if offsets:
        here = lax.axis_index("band")
        firsts = [((here ^ k) * cycles_here, cycles_here) for k in offsets]
        modes = jnp.concatenate([ref[...] for ref in modes_refs], 0)
    else:
        modes = modes_refs[0][...]
        modes = modes.reshape(-1, *modes.shape[2:])
        firsts = [(0, modes.shape[0])]
    left_ref[...], left_high_ref[...] = left_of(
        modes, efficiency_ref[...], orders, efficiency_ref.shape[0] // 2
    )
    return firsts


def prepare_kernel(window_ref, legendre_ref, plus_ref, minus_ref, *refs, orders, cycles_here):
    if len(refs) > 3:
        efficiency_ref, own_ref, *refs, binned_ref, left_ref, left_high_ref = refs
        rows = efficiency_ref.shape[0]
        firsts = gather_left([own_ref], efficiency_ref, left_ref, left_high_ref, orders, cycles_here, (0,))
        own = True
    else:
        own = False
    high_ref, low_ref, tables_ref = refs
    columns = legendre_ref.shape[0] * legendre_ref.shape[1]
    same = jnp.where(iota((TILE, TILE), 0) == iota((TILE, TILE), 1), 1.0, 0.0).astype(jnp.bfloat16)

    def step(start):
        lanes = pl.ds(start, TILE)
        high, low = split(window_ref[:, lanes])
        high_ref[:, lanes], low_ref[:, lanes] = high, low
        tables = [
            *split(legendre_ref[:, :, lanes].reshape(columns, TILE)),
            plus_ref[:, :, lanes].reshape(columns, TILE),
            minus_ref[:, :, lanes].reshape(columns, TILE),
        ]
        tables_ref[lanes, :] = lax.dot_general(
            same, jnp.concatenate(tables, 0), (((1,), (1,)), ((), ())), preferred_element_type=jnp.float32,
        ).astype(jnp.bfloat16)
        if own:
            binned = add_cycles(
                [jnp.zeros((rows, TILE), jnp.float32)] * orders,
                multiply(left_ref[...], left_high_ref[...], high, low), legendre_ref, firsts, lanes, orders, rows,
            )
            for m in range(orders):
                binned_ref[pl.ds(m * rows, rows), lanes] = binned[m]

    each_tile(legendre_ref.shape[2], own, step)


def more_kernel(
    efficiency_ref, legendre_ref, high_ref, low_ref, binned_in, modes_ref, binned_ref, left_ref, left_high_ref,
    *, orders, cycles_here, offset,
):
    rows = efficiency_ref.shape[0]
    firsts = gather_left([modes_ref], efficiency_ref, left_ref, left_high_ref, orders, cycles_here, (offset,))

    def step(start):
        lanes = pl.ds(start, TILE)
        binned = add_cycles(
            [binned_in[pl.ds(m * rows, rows), lanes] for m in range(orders)],
            multiply(left_ref[...], left_high_ref[...], high_ref[:, lanes], low_ref[:, lanes]),
            legendre_ref, firsts, lanes, orders, rows,
        )
        for m in range(orders):
            binned_ref[pl.ds(m * rows, rows), lanes] = binned[m]

    each_tile(legendre_ref.shape[2], True, step)


def maps_kernel(
    efficiency_ref, legendre_ref, high_ref, low_ref, tables_ref, *refs,
    bands, orders, cycles_here, offsets,
):
    if offsets:
        binned_ref, *refs = refs
    *modes_refs, out_ref, left_ref, left_high_ref, sums_ref = refs
    cycles = legendre_ref.shape[1]
    rows = efficiency_ref.shape[0]
    bins = rows // 2
    columns = orders * cycles
    firsts = gather_left(modes_refs, efficiency_ref, left_ref, left_high_ref, orders, cycles_here, offsets)
    sums_ref[...] = jnp.zeros(sums_ref.shape, jnp.float32)

    group = GROUP if offsets else 2

    def coefficients(start, product):
        lanes = pl.ds(start, TILE)
        if offsets:
            binned = [binned_ref[pl.ds(m * rows, rows), lanes] for m in range(orders)]
        else:
            binned = [jnp.zeros((rows, TILE), jnp.float32)] * orders
        binned = add_cycles(binned, product, legendre_ref, firsts, lanes, orders, rows)
        binned = jnp.concatenate(binned, 0)
        degree = (start + iota((rows, TILE), 1)).astype(jnp.float32)
        ratio = jnp.where(
            degree >= 2.0,
            jnp.sqrt((degree + 2.0) * (degree - 1.0) / jnp.maximum(degree * (degree + 1.0), 1.0)),
            0.0,
        )
        shear = (-jnp.concatenate([ratio] * orders, 0) * binned).astype(jnp.bfloat16)
        high, low = split(binned)
        return jnp.concatenate([high, low, shear], 0)

    def step(start):
        starts = [start + i * TILE for i in range(group)]
        spans = [pl.ds(at, TILE) for at in starts]
        products = [
            multiply(left_ref[...], left_high_ref[...], high_ref[:, lanes], low_ref[:, lanes]) for lanes in spans
        ]
        lefts = [coefficients(*pair) for pair in zip(starts, products)]
        parts = [
            jnp.dot(left, tables_ref[lanes, :], preferred_element_type=jnp.float32)
            for left, lanes in zip(lefts, spans)
        ]
        sums_ref[...] += sum(parts[1:], parts[0])

    each_tile(legendre_ref.shape[2], bool(offsets), step, group * TILE)

    lane = iota((rows, 4 * columns), 1)
    table = lane // columns
    order = lane % columns // cycles

    def own(kind):
        total = jnp.zeros((rows, 4 * columns), jnp.float32)
        for m in range(orders):
            total = jnp.where(order == m, sums_ref[pl.ds((kind * orders + m) * rows, rows), :], total)
        return total

    kappa = own(0) + jnp.where(table == KAPPA_HIGH, own(1), 0.0)
    value = jnp.where(table < PLUS, kappa, own(2))
    count = 4 * columns // LANES
    slot = iota((rows, LANES), 1) % cycles // cycles_here
    shifted = {}
    for z in range(bands):
        halves = []
        for c in range(2):
            half = jnp.zeros((rows, LANES), jnp.float32)
            for v in range(count):
                at = c * count + v
                shift = (at - z) * cycles_here % LANES
                if (v, shift) not in shifted:
                    part = value[:, v * LANES : (v + 1) * LANES]
                    shifted[v, shift] = pltpu.roll(part, shift, 1) if shift else part
                half = jnp.where(slot == at, shifted[v, shift], half)
            halves.append(half)
        row = jnp.where(slot[:bins] < count, halves[0][:bins], halves[1][bins:])
        for b in range(bins):
            out_ref[b * bands + z] = row[b : b + 1]


def unpack_kernel(got_ref, out_ref, *, bands, orders, cycles_here):
    groups = got_ref.shape[0] // bands
    cycles = bands * cycles_here
    columns = orders * cycles
    count = 4 * columns // LANES

    def origin(lane):
        slot = lane % cycles // cycles_here
        source = slot % count * LANES + lane // cycles * cycles
        return slot // count, source // columns, source % columns // cycles

    shape = (orders, LANES)
    own_order = origin(iota(shape, 1))[2] == iota(shape, 0)
    values = []
    for z in range(bands):
        total = got_ref[z]
        for p in range(1, groups):
            total = total + got_ref[p * bands + z]
        values.append(jnp.where(own_order, jnp.broadcast_to(total, shape), 0.0))
    shape = (3 * cycles_here * 2, LANES)
    row, lane = iota(shape, 0), iota(shape, 1)
    field, cycle, part = row // (2 * cycles_here), row // 2 % cycles_here, row % 2
    lane_part, table, _ = origin(lane)
    same = jnp.where(lane_part == part, 1.0, 0.0)
    other = jnp.where(lane_part == part, 0.0, jnp.where(part == 0, -1.0, 1.0))
    pick = jnp.where(
        field == 0,
        jnp.where(table <= KAPPA_LOW, same, 0.0),
        jnp.where(field == 1, jnp.where(table == PLUS, same, 0.0), jnp.where(table == MINUS, other, 0.0)),
    )
    maps = lax.dot_general(
        jnp.where(lane % cycles_here == cycle, pick, 0.0), jnp.concatenate(values, 0), (((1,), (1,)), ((), ())),
        precision=lax.Precision.HIGHEST, preferred_element_type=jnp.float32,
    )
    for i in range(3 * cycles_here):
        out_ref[i] = maps[2 * i : 2 * i + 2]


def on_device(
    cycle_modes, cycle_weight, legendre, spin_plus, spin_minus, window, lensing, source_shell
):
    bands = lax.axis_size("band")
    shell_parts = lax.axis_size("shell")
    shells, cycles_here, _, orders_all = cycle_modes.shape
    orders, cycles, degrees = legendre.shape
    bins = source_shell.shape[0]
    assert bins == shell_parts and 8 * orders * cycles_here == LANES
    offsets = (2, 3, 1) if bands == 4 else ()
    rows = 2 * bins
    columns = 4 * orders * cycles

    def shaped(*shape, dtype=jnp.float32):
        return jax.ShapeDtypeStruct(shape, dtype)

    def left_scratch(blocks):
        return [
            pltpu.VMEM((orders * blocks * cycles_here * rows, 2 * shells), jnp.bfloat16),
            pltpu.VMEM((orders * blocks * cycles_here * rows, shells), jnp.bfloat16),
        ]

    block_shape = (cycles_here, 2 * orders, shells)
    out_shape = [shaped(*block_shape)] * bands if offsets else [shaped(bands, *block_shape)]
    out_shape = [*out_shape, shaped(rows, shells)]
    sources = (
        cycle_modes.transpose(1, 2, 3, 0), cycle_weight.reshape(1, cycles_here),
        source_shell.reshape(1, bins), lensing.reshape(1, shells),
    )
    sources = pl.pallas_call(
        load_kernel,
        in_specs=[HBM] * 4,
        out_specs=[VMEM] * 4,
        out_shape=[shaped(*x.shape, dtype=x.dtype) for x in sources],
        scratch_shapes=[pltpu.SemaphoreType.DMA((4,))],
        compiler_params=PARAMS,
        name="load",
    )(*map(keep, sources))
    *blocks, efficiency = pl.pallas_call(
        functools.partial(pack_kernel, bands=bands, orders=orders, bins=bins, offsets=offsets),
        in_specs=[VMEM] * 4,
        out_specs=[VMEM] * len(out_shape),
        out_shape=out_shape,
        scratch_shapes=[pltpu.VMEM((bands, *block_shape), jnp.float32)],
        compiler_params=PARAMS,
        cost_estimate=pl.CostEstimate(flops=10**10, bytes_accessed=2**17, transcendentals=0),
        name="pack",
    )(*sources)
    if offsets:
        own, *sends = blocks
        got = [
            lax.ppermute(send, "band", [(z, z ^ k) for z in range(bands)])
            for k, send in zip(offsets, sends)
        ]
    else:
        got = [lax.all_to_all(blocks[0], "band", split_axis=0, concat_axis=0, tiled=True)]
    half = jnp.bfloat16
    tables = [shaped(shells, degrees, dtype=half)] * 2 + [shaped(degrees, columns, dtype=half)]
    binned_shape = shaped(orders * rows, degrees)
    arguments = [window, legendre, spin_plus, spin_minus]
    if offsets:
        tables.append(binned_shape)
        arguments += [efficiency, own]
    high, low, turned, *binned = pl.pallas_call(
        functools.partial(prepare_kernel, orders=orders, cycles_here=cycles_here),
        in_specs=[VMEM] * len(arguments),
        out_specs=[VMEM] * len(tables),
        out_shape=tables,
        scratch_shapes=left_scratch(1) if offsets else [],
        compiler_params=PARAMS,
        name="prepare",
    )(*arguments)
    for k, block in zip(offsets[:-1], got):
        binned = [
            pl.pallas_call(
                functools.partial(more_kernel, orders=orders, cycles_here=cycles_here, offset=k),
                in_specs=[VMEM] * 6,
                out_specs=VMEM,
                out_shape=binned_shape,
                scratch_shapes=left_scratch(1),
                compiler_params=PARAMS,
                name="more",
            )(efficiency, legendre, high, low, *binned, block)
        ]
    last = got[-1:]
    operands = [efficiency, legendre, high, low, turned, *binned, *last]
    maps = pl.pallas_call(
        functools.partial(
            maps_kernel, bands=bands, orders=orders, cycles_here=cycles_here, offsets=offsets[-1:]
        ),
        in_specs=[VMEM] * len(operands),
        out_specs=VMEM,
        out_shape=shaped(bins * bands, 1, LANES),
        scratch_shapes=[
            *left_scratch(len(last) if offsets else bands),
            pltpu.VMEM((3 * orders * rows, columns), jnp.float32),
        ],
        compiler_params=PARAMS,
        name="maps",
    )(*operands)
    got = lax.all_to_all(maps, ("shell", "band"), split_axis=0, concat_axis=0, tiled=True)
    out = pl.pallas_call(
        functools.partial(unpack_kernel, bands=bands, orders=orders, cycles_here=cycles_here),
        in_specs=[VMEM],
        out_specs=VMEM,
        out_shape=shaped(3 * cycles_here, 2, orders_all),
        compiler_params=PARAMS,
        name="unpack",
    )(got)
    return out.reshape(1, 3, cycles_here, 2, orders_all)


def solution(mesh):
    placed = (
        P(("cosmo", "shell"), "band", None, None),
        P("band"),
        P("band", None, None),
        P("band", None, None),
        P("band", None, None),
        P("shell", None),
        P(("cosmo", "shell")),
        P("cosmo"),
    )
    return jax.shard_map(
        on_device,
        mesh=mesh,
        in_specs=placed,
        out_specs=P(("cosmo", "shell"), None, "band", None, None),
        check_vma=False,
    )
```

```python
import functools

import jax
import jax.numpy as jnp
from jax import lax
from jax.experimental import pallas as pl
from jax.experimental.pallas import tpu as pltpu
from jax.sharding import PartitionSpec as P

TILE = 256
GROUP = 16
LANES = 128
ROUTES = ((0, 1, 2, 3), (2, 3, 1, 0), (1, 0, 3, 2), (3, 2, 0, 1))
VMEM = pl.BlockSpec(memory_space=pltpu.VMEM)
HBM = pl.BlockSpec(memory_space=pltpu.HBM)
PARAMS = pltpu.CompilerParams(vmem_limit_bytes=28 * 2**20)
KAPPA_HIGH, KAPPA_LOW, PLUS, MINUS = range(4)


def keep(x):
    return pltpu.with_memory_space_constraint(x, pltpu.HBM)


def route(k, here, back=False):
    bands = range(len(ROUTES[k]))
    ends = tuple(ROUTES[k].index(z) for z in bands) if back else ROUTES[k]
    end = jnp.int32(ends[0])
    for z in bands[1:]:
        end = jnp.where(here == z, ends[z], end)
    return end


def split(x):
    high = x.astype(jnp.bfloat16)
    low = (x - high.astype(jnp.float32)).astype(jnp.bfloat16)
    return high, low


def iota(shape, axis):
    return lax.broadcasted_iota(jnp.int32, shape, axis)


def load_kernel(*refs):
    count = len(refs) // 2
    copies = [pltpu.make_async_copy(refs[i], refs[count + i], refs[-1].at[i]) for i in range(count)]
    for copy in copies:
        copy.start()
    for copy in copies:
        copy.wait()


def pack_kernel(modes_ref, weight_ref, source_ref, lensing_ref, *refs, bands, orders, bins, offsets):
    *out_refs, efficiency_ref, blocks_ref = refs
    cycles_here, _, _, shells = modes_ref.shape
    for r in range(cycles_here):
        weight = jnp.broadcast_to(weight_ref[0:1, r : r + 1], (orders, shells))
        for c in range(2):
            for z in range(bands):
                blocks_ref[z, r, c * orders : (c + 1) * orders, :] = (
                    modes_ref[r, c, z * orders : (z + 1) * orders, :] * weight
                )
    if offsets:
        here = lax.axis_index("band")
        for k, out_ref in zip((0, *offsets), out_refs):
            out_ref[...] = blocks_ref[route(k, here)]
    else:
        out_refs[0][...] = blocks_ref[...]
    rows = 2 * bins
    row_bin = iota((rows, shells), 0) % bins
    source = jnp.zeros((rows, shells), jnp.int32)
    for b in range(bins):
        source = jnp.where(row_bin == b, jnp.broadcast_to(source_ref[0:1, b : b + 1], (rows, shells)), source)
    shell_ids = lax.axis_index("shell") * shells + iota((rows, shells), 1)
    efficiency_ref[...] = (
        lensing_ref[...]
        * jnp.maximum(source - shell_ids, 0).astype(jnp.float32)
        / (source + 1).astype(jnp.float32)
    )


def left_of(modes, efficiency, orders, bins):
    cycles, _, shells = modes.shape
    rows = 2 * bins
    first_part = (iota((1, rows, shells), 1) < bins)
    parts = []
    for m in range(orders):
        real = jnp.broadcast_to(modes[:, m : m + 1, :], (cycles, rows, shells))
        imag = jnp.broadcast_to(modes[:, orders + m : orders + m + 1, :], (cycles, rows, shells))
        left = jnp.where(first_part, real, imag) * efficiency[None]
        parts.append(left.reshape(cycles * rows, shells))
    high, low = split(jnp.concatenate(parts, 0))
    return jnp.concatenate([high, low], 1), high


def multiply(left, left_high, high, low):
    product = jnp.dot(left, jnp.concatenate([high, high], 0), preferred_element_type=jnp.float32)
    return product + jnp.dot(left_high, low, preferred_element_type=jnp.float32)


def add_cycles(binned, product, legendre_ref, firsts, lanes, orders, rows):
    out = []
    at = 0
    for m in range(orders):
        total = binned[m]
        for first, count in firsts:
            for r in range(count):
                total = total + legendre_ref[m, pl.ds(first + r, 1), lanes] * product[at : at + rows]
                at += rows
        out.append(total)
    return out


def each_tile(degrees, unroll, step, size=TILE):
    if unroll:
        for start in range(0, degrees, size):
            step(start)
    else:
        pl.loop(0, degrees // size)(lambda i: step(pl.multiple_of(i * size, size)))


def gather_left(modes_refs, efficiency_ref, left_ref, left_high_ref, orders, cycles_here, offsets):
    if offsets:
        here = lax.axis_index("band")
        firsts = [(route(k, here, True) * cycles_here, cycles_here) for k in offsets]
        modes = jnp.concatenate([ref[...] for ref in modes_refs], 0)
    else:
        modes = modes_refs[0][...]
        modes = modes.reshape(-1, *modes.shape[2:])
        firsts = [(0, modes.shape[0])]
    left_ref[...], left_high_ref[...] = left_of(
        modes, efficiency_ref[...], orders, efficiency_ref.shape[0] // 2
    )
    return firsts


def prepare_kernel(window_ref, legendre_ref, plus_ref, minus_ref, *refs, orders, cycles_here):
    if len(refs) > 3:
        efficiency_ref, own_ref, *refs, binned_ref, left_ref, left_high_ref = refs
        rows = efficiency_ref.shape[0]
        firsts = gather_left([own_ref], efficiency_ref, left_ref, left_high_ref, orders, cycles_here, (0,))
        own = True
    else:
        own = False
    high_ref, low_ref, tables_ref = refs
    columns = legendre_ref.shape[0] * legendre_ref.shape[1]
    same = jnp.where(iota((TILE, TILE), 0) == iota((TILE, TILE), 1), 1.0, 0.0).astype(jnp.bfloat16)

    def step(start):
        lanes = pl.ds(start, TILE)
        high, low = split(window_ref[:, lanes])
        high_ref[:, lanes], low_ref[:, lanes] = high, low
        tables = [
            *split(legendre_ref[:, :, lanes].reshape(columns, TILE)),
            plus_ref[:, :, lanes].reshape(columns, TILE),
            minus_ref[:, :, lanes].reshape(columns, TILE),
        ]
        tables_ref[lanes, :] = lax.dot_general(
            same, jnp.concatenate(tables, 0), (((1,), (1,)), ((), ())), preferred_element_type=jnp.float32,
        ).astype(jnp.bfloat16)
        if own:
            binned = add_cycles(
                [jnp.zeros((rows, TILE), jnp.float32)] * orders,
                multiply(left_ref[...], left_high_ref[...], high, low), legendre_ref, firsts, lanes, orders, rows,
            )
            for m in range(orders):
                binned_ref[pl.ds(m * rows, rows), lanes] = binned[m]

    each_tile(legendre_ref.shape[2], own, step)


def more_kernel(
    efficiency_ref, legendre_ref, high_ref, low_ref, binned_in, modes_ref, binned_ref, left_ref, left_high_ref,
    *, orders, cycles_here, offset,
):
    rows = efficiency_ref.shape[0]
    firsts = gather_left([modes_ref], efficiency_ref, left_ref, left_high_ref, orders, cycles_here, (offset,))

    def step(start):
        lanes = pl.ds(start, TILE)
        binned = add_cycles(
            [binned_in[pl.ds(m * rows, rows), lanes] for m in range(orders)],
            multiply(left_ref[...], left_high_ref[...], high_ref[:, lanes], low_ref[:, lanes]),
            legendre_ref, firsts, lanes, orders, rows,
        )
        for m in range(orders):
            binned_ref[pl.ds(m * rows, rows), lanes] = binned[m]

    each_tile(legendre_ref.shape[2], True, step)


def maps_kernel(
    efficiency_ref, legendre_ref, high_ref, low_ref, tables_ref, *refs,
    bands, orders, cycles_here, offsets,
):
    if offsets:
        binned_ref, *refs = refs
    *modes_refs, out_ref, left_ref, left_high_ref, sums_ref = refs
    cycles = legendre_ref.shape[1]
    rows = efficiency_ref.shape[0]
    bins = rows // 2
    columns = orders * cycles
    firsts = gather_left(modes_refs, efficiency_ref, left_ref, left_high_ref, orders, cycles_here, offsets)
    sums_ref[...] = jnp.zeros(sums_ref.shape, jnp.float32)

    group = GROUP if offsets else 2

    def coefficients(start, product):
        lanes = pl.ds(start, TILE)
        if offsets:
            binned = [binned_ref[pl.ds(m * rows, rows), lanes] for m in range(orders)]
        else:
            binned = [jnp.zeros((rows, TILE), jnp.float32)] * orders
        binned = add_cycles(binned, product, legendre_ref, firsts, lanes, orders, rows)
        binned = jnp.concatenate(binned, 0)
        degree = (start + iota((rows, TILE), 1)).astype(jnp.float32)
        ratio = jnp.where(
            degree >= 2.0,
            jnp.sqrt((degree + 2.0) * (degree - 1.0) / jnp.maximum(degree * (degree + 1.0), 1.0)),
            0.0,
        )
        shear = (-jnp.concatenate([ratio] * orders, 0) * binned).astype(jnp.bfloat16)
        high, low = split(binned)
        return jnp.concatenate([high, low, shear], 0)

    def step(start):
        starts = [start + i * TILE for i in range(group)]
        spans = [pl.ds(at, TILE) for at in starts]
        products = [
            multiply(left_ref[...], left_high_ref[...], high_ref[:, lanes], low_ref[:, lanes]) for lanes in spans
        ]
        lefts = [coefficients(*pair) for pair in zip(starts, products)]
        parts = [
            jnp.dot(left, tables_ref[lanes, :], preferred_element_type=jnp.float32)
            for left, lanes in zip(lefts, spans)
        ]
        sums_ref[...] += sum(parts[1:], parts[0])

    each_tile(legendre_ref.shape[2], bool(offsets), step, group * TILE)

    lane = iota((rows, 4 * columns), 1)
    table = lane // columns
    order = lane % columns // cycles

    def own(kind):
        total = jnp.zeros((rows, 4 * columns), jnp.float32)
        for m in range(orders):
            total = jnp.where(order == m, sums_ref[pl.ds((kind * orders + m) * rows, rows), :], total)
        return total

    kappa = own(0) + jnp.where(table == KAPPA_HIGH, own(1), 0.0)
    value = jnp.where(table < PLUS, kappa, own(2))
    count = 4 * columns // LANES
    slot = iota((rows, LANES), 1) % cycles // cycles_here
    shifted = {}
    for z in range(bands):
        halves = []
        for c in range(2):
            half = jnp.zeros((rows, LANES), jnp.float32)
            for v in range(count):
                at = c * count + v
                shift = (at - z) * cycles_here % LANES
                if (v, shift) not in shifted:
                    part = value[:, v * LANES : (v + 1) * LANES]
                    shifted[v, shift] = pltpu.roll(part, shift, 1) if shift else part
                half = jnp.where(slot == at, shifted[v, shift], half)
            halves.append(half)
        row = jnp.where(slot[:bins] < count, halves[0][:bins], halves[1][bins:])
        for b in range(bins):
            out_ref[b * bands + z] = row[b : b + 1]


def unpack_kernel(got_ref, out_ref, *, bands, orders, cycles_here):
    groups = got_ref.shape[0] // bands
    cycles = bands * cycles_here
    columns = orders * cycles
    count = 4 * columns // LANES

    def origin(lane):
        slot = lane % cycles // cycles_here
        source = slot % count * LANES + lane // cycles * cycles
        return slot // count, source // columns, source % columns // cycles

    shape = (orders, LANES)
    own_order = origin(iota(shape, 1))[2] == iota(shape, 0)
    values = []
    for z in range(bands):
        total = got_ref[z]
        for p in range(1, groups):
            total = total + got_ref[p * bands + z]
        values.append(jnp.where(own_order, jnp.broadcast_to(total, shape), 0.0))
    shape = (3 * cycles_here * 2, LANES)
    row, lane = iota(shape, 0), iota(shape, 1)
    field, cycle, part = row // (2 * cycles_here), row // 2 % cycles_here, row % 2
    lane_part, table, _ = origin(lane)
    same = jnp.where(lane_part == part, 1.0, 0.0)
    other = jnp.where(lane_part == part, 0.0, jnp.where(part == 0, -1.0, 1.0))
    pick = jnp.where(
        field == 0,
        jnp.where(table <= KAPPA_LOW, same, 0.0),
        jnp.where(field == 1, jnp.where(table == PLUS, same, 0.0), jnp.where(table == MINUS, other, 0.0)),
    )
    maps = lax.dot_general(
        jnp.where(lane % cycles_here == cycle, pick, 0.0), jnp.concatenate(values, 0), (((1,), (1,)), ((), ())),
        precision=lax.Precision.HIGHEST, preferred_element_type=jnp.float32,
    )
    for i in range(3 * cycles_here):
        out_ref[i] = maps[2 * i : 2 * i + 2]


def on_device(
    cycle_modes, cycle_weight, legendre, spin_plus, spin_minus, window, lensing, source_shell
):
    bands = lax.axis_size("band")
    shell_parts = lax.axis_size("shell")
    shells, cycles_here, _, orders_all = cycle_modes.shape
    orders, cycles, degrees = legendre.shape
    bins = source_shell.shape[0]
    assert bins == shell_parts and 8 * orders * cycles_here == LANES
    offsets = tuple(range(1, bands)) if bands == len(ROUTES) else ()
    rows = 2 * bins
    columns = 4 * orders * cycles

    def shaped(*shape, dtype=jnp.float32):
        return jax.ShapeDtypeStruct(shape, dtype)

    def left_scratch(blocks):
        return [
            pltpu.VMEM((orders * blocks * cycles_here * rows, 2 * shells), jnp.bfloat16),
            pltpu.VMEM((orders * blocks * cycles_here * rows, shells), jnp.bfloat16),
        ]

    block_shape = (cycles_here, 2 * orders, shells)
    out_shape = [shaped(*block_shape)] * bands if offsets else [shaped(bands, *block_shape)]
    out_shape = [*out_shape, shaped(rows, shells)]
    sources = (
        cycle_modes.transpose(1, 2, 3, 0), cycle_weight.reshape(1, cycles_here),
        source_shell.reshape(1, bins), lensing.reshape(1, shells),
    )
    sources = pl.pallas_call(
        load_kernel,
        in_specs=[HBM] * 4,
        out_specs=[VMEM] * 4,
        out_shape=[shaped(*x.shape, dtype=x.dtype) for x in sources],
        scratch_shapes=[pltpu.SemaphoreType.DMA((4,))],
        compiler_params=PARAMS,
        name="load",
    )(*map(keep, sources))
    *blocks, efficiency = pl.pallas_call(
        functools.partial(pack_kernel, bands=bands, orders=orders, bins=bins, offsets=offsets),
        in_specs=[VMEM] * 4,
        out_specs=[VMEM] * len(out_shape),
        out_shape=out_shape,
        scratch_shapes=[pltpu.VMEM((bands, *block_shape), jnp.float32)],
        compiler_params=PARAMS,
        cost_estimate=pl.CostEstimate(flops=10**10, bytes_accessed=2**17, transcendentals=0),
        name="pack",
    )(*sources)
    if offsets:
        own, *sends = blocks
        got = [
            lax.ppermute(send, "band", [(z, ROUTES[k][z]) for z in range(bands)])
            for k, send in zip(offsets, sends)
        ]
    else:
        got = [lax.all_to_all(blocks[0], "band", split_axis=0, concat_axis=0, tiled=True)]
    half = jnp.bfloat16
    tables = [shaped(shells, degrees, dtype=half)] * 2 + [shaped(degrees, columns, dtype=half)]
    binned_shape = shaped(orders * rows, degrees)
    arguments = [window, legendre, spin_plus, spin_minus]
    if offsets:
        tables.append(binned_shape)
        arguments += [efficiency, own]
    high, low, turned, *binned = pl.pallas_call(
        functools.partial(prepare_kernel, orders=orders, cycles_here=cycles_here),
        in_specs=[VMEM] * len(arguments),
        out_specs=[VMEM] * len(tables),
        out_shape=tables,
        scratch_shapes=left_scratch(1) if offsets else [],
        compiler_params=PARAMS,
        name="prepare",
    )(*arguments)
    for k, block in zip(offsets[:-1], got):
        binned = [
            pl.pallas_call(
                functools.partial(more_kernel, orders=orders, cycles_here=cycles_here, offset=k),
                in_specs=[VMEM] * 6,
                out_specs=VMEM,
                out_shape=binned_shape,
                scratch_shapes=left_scratch(1),
                compiler_params=PARAMS,
                name="more",
            )(efficiency, legendre, high, low, *binned, block)
        ]
    last = got[-1:]
    operands = [efficiency, legendre, high, low, turned, *binned, *last]
    maps = pl.pallas_call(
        functools.partial(
            maps_kernel, bands=bands, orders=orders, cycles_here=cycles_here, offsets=offsets[-1:]
        ),
        in_specs=[VMEM] * len(operands),
        out_specs=VMEM,
        out_shape=shaped(bins * bands, 1, LANES),
        scratch_shapes=[
            *left_scratch(len(last) if offsets else bands),
            pltpu.VMEM((3 * orders * rows, columns), jnp.float32),
        ],
        compiler_params=PARAMS,
        name="maps",
    )(*operands)
    got = lax.all_to_all(maps, ("shell", "band"), split_axis=0, concat_axis=0, tiled=True)
    out = pl.pallas_call(
        functools.partial(unpack_kernel, bands=bands, orders=orders, cycles_here=cycles_here),
        in_specs=[VMEM],
        out_specs=VMEM,
        out_shape=shaped(3 * cycles_here, 2, orders_all),
        compiler_params=PARAMS,
        name="unpack",
    )(got)
    return out.reshape(1, 3, cycles_here, 2, orders_all)


def solution(mesh):
    placed = (
        P(("cosmo", "shell"), "band", None, None),
        P("band"),
        P("band", None, None),
        P("band", None, None),
        P("band", None, None),
        P("shell", None),
        P(("cosmo", "shell")),
        P("cosmo"),
    )
    return jax.shard_map(
        on_device,
        mesh=mesh,
        in_specs=placed,
        out_specs=P(("cosmo", "shell"), None, "band", None, None),
        check_vma=False,
    )
```

```python
import functools

import jax
import jax.numpy as jnp
from jax import lax
from jax.experimental import pallas as pl
from jax.experimental.pallas import tpu as pltpu
from jax.sharding import PartitionSpec as P

TILE = 256
GROUP = 16
LANES = 128
ROUTES = ((0, 1, 2, 3), (2, 3, 1, 0), (1, 0, 3, 2), (3, 2, 0, 1))
VMEM = pl.BlockSpec(memory_space=pltpu.VMEM)
HBM = pl.BlockSpec(memory_space=pltpu.HBM)
PARAMS = pltpu.CompilerParams(vmem_limit_bytes=28 * 2**20)
KAPPA_HIGH, KAPPA_LOW, PLUS, MINUS = range(4)


def keep(x):
    return pltpu.with_memory_space_constraint(x, pltpu.HBM)


def route(k, here, back=False):
    bands = range(len(ROUTES[k]))
    ends = tuple(ROUTES[k].index(z) for z in bands) if back else ROUTES[k]
    end = jnp.int32(ends[0])
    for z in bands[1:]:
        end = jnp.where(here == z, ends[z], end)
    return end


def split(x):
    high = x.astype(jnp.bfloat16)
    low = (x - high.astype(jnp.float32)).astype(jnp.bfloat16)
    return high, low


def iota(shape, axis):
    return lax.broadcasted_iota(jnp.int32, shape, axis)


def load_kernel(*refs):
    count = len(refs) // 2
    copies = [pltpu.make_async_copy(refs[i], refs[count + i], refs[-1].at[i]) for i in range(count)]
    for copy in copies:
        copy.start()
    for copy in copies:
        copy.wait()


def pack_kernel(modes_ref, weight_ref, source_ref, lensing_ref, *refs, bands, orders, bins, offsets):
    *out_refs, efficiency_ref, blocks_ref = refs
    cycles_here, _, _, shells = modes_ref.shape
    for r in range(cycles_here):
        weight = jnp.broadcast_to(weight_ref[0:1, r : r + 1], (orders, shells))
        for c in range(2):
            for z in range(bands):
                blocks_ref[z, r, c * orders : (c + 1) * orders, :] = (
                    modes_ref[r, c, z * orders : (z + 1) * orders, :] * weight
                )
    if offsets:
        here = lax.axis_index("band")
        for k, out_ref in zip((0, *offsets), out_refs):
            out_ref[...] = blocks_ref[route(k, here)]
    else:
        out_refs[0][...] = blocks_ref[...]
    rows = 2 * bins
    row_bin = iota((rows, shells), 0) % bins
    source = jnp.zeros((rows, shells), jnp.int32)
    for b in range(bins):
        source = jnp.where(row_bin == b, jnp.broadcast_to(source_ref[0:1, b : b + 1], (rows, shells)), source)
    shell_ids = lax.axis_index("shell") * shells + iota((rows, shells), 1)
    efficiency_ref[...] = (
        lensing_ref[...]
        * jnp.maximum(source - shell_ids, 0).astype(jnp.float32)
        / (source + 1).astype(jnp.float32)
    )


def left_of(modes, efficiency, orders, bins):
    cycles, _, shells = modes.shape
    rows = 2 * bins
    first_part = (iota((1, rows, shells), 1) < bins)
    parts = []
    for m in range(orders):
        real = jnp.broadcast_to(modes[:, m : m + 1, :], (cycles, rows, shells))
        imag = jnp.broadcast_to(modes[:, orders + m : orders + m + 1, :], (cycles, rows, shells))
        left = jnp.where(first_part, real, imag) * efficiency[None]
        parts.append(left.reshape(cycles * rows, shells))
    high, low = split(jnp.concatenate(parts, 0))
    return jnp.concatenate([high, low], 1), high


def multiply(left, left_high, high, low):
    product = jnp.dot(left, jnp.concatenate([high, high], 0), preferred_element_type=jnp.float32)
    return product + jnp.dot(left_high, low, preferred_element_type=jnp.float32)


def add_cycles(binned, product, legendre_ref, firsts, lanes, orders, rows):
    out = []
    at = 0
    for m in range(orders):
        total = binned[m]
        for first, count in firsts:
            for r in range(count):
                total = total + legendre_ref[m, pl.ds(first + r, 1), lanes] * product[at : at + rows]
                at += rows
        out.append(total)
    return out


def each_tile(degrees, unroll, step, size=TILE):
    if unroll:
        for start in range(0, degrees, size):
            step(start)
    else:
        pl.loop(0, degrees // size)(lambda i: step(pl.multiple_of(i * size, size)))


def gather_left(modes_refs, efficiency_ref, left_ref, left_high_ref, orders, cycles_here, offsets):
    if offsets:
        here = lax.axis_index("band")
        firsts = [(route(k, here, True) * cycles_here, cycles_here) for k in offsets]
        modes = jnp.concatenate([ref[...] for ref in modes_refs], 0)
    else:
        modes = modes_refs[0][...]
        modes = modes.reshape(-1, *modes.shape[2:])
        firsts = [(0, modes.shape[0])]
    left_ref[...], left_high_ref[...] = left_of(
        modes, efficiency_ref[...], orders, efficiency_ref.shape[0] // 2
    )
    return firsts


def prepare_kernel(window_ref, legendre_ref, plus_ref, minus_ref, *refs, orders, cycles_here):
    if len(refs) > 3:
        efficiency_ref, own_ref, *refs, binned_ref, left_ref, left_high_ref = refs
        rows = efficiency_ref.shape[0]
        firsts = gather_left([own_ref], efficiency_ref, left_ref, left_high_ref, orders, cycles_here, (0,))
        own = True
    else:
        own = False
    high_ref, low_ref, tables_ref = refs
    columns = legendre_ref.shape[0] * legendre_ref.shape[1]
    same = jnp.where(iota((TILE, TILE), 0) == iota((TILE, TILE), 1), 1.0, 0.0).astype(jnp.bfloat16)

    def step(start):
        lanes = pl.ds(start, TILE)
        high, low = split(window_ref[:, lanes])
        high_ref[:, lanes], low_ref[:, lanes] = high, low
        tables = [
            *split(legendre_ref[:, :, lanes].reshape(columns, TILE)),
            plus_ref[:, :, lanes].reshape(columns, TILE),
            minus_ref[:, :, lanes].reshape(columns, TILE),
        ]
        tables_ref[lanes, :] = lax.dot_general(
            same, jnp.concatenate(tables, 0), (((1,), (1,)), ((), ())), preferred_element_type=jnp.float32,
        ).astype(jnp.bfloat16)
        if own:
            binned = add_cycles(
                [jnp.zeros((rows, TILE), jnp.float32)] * orders,
                multiply(left_ref[...], left_high_ref[...], high, low), legendre_ref, firsts, lanes, orders, rows,
            )
            for m in range(orders):
                binned_ref[pl.ds(m * rows, rows), lanes] = binned[m]

    each_tile(legendre_ref.shape[2], own, step)


def more_kernel(
    efficiency_ref, legendre_ref, high_ref, low_ref, binned_in, modes_ref, binned_ref, left_ref, left_high_ref,
    *, orders, cycles_here, offset,
):
    rows = efficiency_ref.shape[0]
    firsts = gather_left([modes_ref], efficiency_ref, left_ref, left_high_ref, orders, cycles_here, (offset,))

    def step(start):
        lanes = pl.ds(start, TILE)
        binned = add_cycles(
            [binned_in[pl.ds(m * rows, rows), lanes] for m in range(orders)],
            multiply(left_ref[...], left_high_ref[...], high_ref[:, lanes], low_ref[:, lanes]),
            legendre_ref, firsts, lanes, orders, rows,
        )
        for m in range(orders):
            binned_ref[pl.ds(m * rows, rows), lanes] = binned[m]

    each_tile(legendre_ref.shape[2], True, step)


def maps_kernel(
    efficiency_ref, legendre_ref, high_ref, low_ref, tables_ref, *refs,
    bands, orders, cycles_here, offsets,
):
    if offsets:
        binned_ref, *refs = refs
    *modes_refs, out_ref, left_ref, left_high_ref, sums_ref = refs
    cycles = legendre_ref.shape[1]
    rows = efficiency_ref.shape[0]
    bins = rows // 2
    columns = orders * cycles
    firsts = gather_left(modes_refs, efficiency_ref, left_ref, left_high_ref, orders, cycles_here, offsets)
    sums_ref[...] = jnp.zeros(sums_ref.shape, jnp.float32)

    group = GROUP if offsets else 2

    def coefficients(start, product):
        lanes = pl.ds(start, TILE)
        if offsets:
            binned = [binned_ref[pl.ds(m * rows, rows), lanes] for m in range(orders)]
        else:
            binned = [jnp.zeros((rows, TILE), jnp.float32)] * orders
        binned = add_cycles(binned, product, legendre_ref, firsts, lanes, orders, rows)
        binned = jnp.concatenate(binned, 0)
        degree = (start + iota((rows, TILE), 1)).astype(jnp.float32)
        ratio = jnp.where(
            degree >= 2.0,
            jnp.sqrt((degree + 2.0) * (degree - 1.0) / jnp.maximum(degree * (degree + 1.0), 1.0)),
            0.0,
        )
        shear = (-jnp.concatenate([ratio] * orders, 0) * binned).astype(jnp.bfloat16)
        high, low = split(binned)
        return jnp.concatenate([high, low, shear], 0)

    def step(start):
        starts = [start + i * TILE for i in range(group)]
        spans = [pl.ds(at, TILE) for at in starts]
        products = [
            multiply(left_ref[...], left_high_ref[...], high_ref[:, lanes], low_ref[:, lanes]) for lanes in spans
        ]
        lefts = [coefficients(*pair) for pair in zip(starts, products)]
        sums_ref[...] += jnp.dot(
            jnp.concatenate(lefts, 1), tables_ref[pl.ds(start, group * TILE), :], preferred_element_type=jnp.float32
        )

    each_tile(legendre_ref.shape[2], bool(offsets), step, group * TILE)

    lane = iota((rows, 4 * columns), 1)
    table = lane // columns
    order = lane % columns // cycles

    def own(kind):
        total = jnp.zeros((rows, 4 * columns), jnp.float32)
        for m in range(orders):
            total = jnp.where(order == m, sums_ref[pl.ds((kind * orders + m) * rows, rows), :], total)
        return total

    kappa = own(0) + jnp.where(table == KAPPA_HIGH, own(1), 0.0)
    value = jnp.where(table < PLUS, kappa, own(2))
    count = 4 * columns // LANES
    slot = iota((rows, LANES), 1) % cycles // cycles_here
    shifted = {}
    for z in range(bands):
        halves = []
        for c in range(2):
            half = jnp.zeros((rows, LANES), jnp.float32)
            for v in range(count):
                at = c * count + v
                shift = (at - z) * cycles_here % LANES
                if (v, shift) not in shifted:
                    part = value[:, v * LANES : (v + 1) * LANES]
                    shifted[v, shift] = pltpu.roll(part, shift, 1) if shift else part
                half = jnp.where(slot == at, shifted[v, shift], half)
            halves.append(half)
        row = jnp.where(slot[:bins] < count, halves[0][:bins], halves[1][bins:])
        for b in range(bins):
            out_ref[b * bands + z] = row[b : b + 1]


def unpack_kernel(got_ref, out_ref, *, bands, orders, cycles_here):
    groups = got_ref.shape[0] // bands
    cycles = bands * cycles_here
    columns = orders * cycles
    count = 4 * columns // LANES

    def origin(lane):
        slot = lane % cycles // cycles_here
        source = slot % count * LANES + lane // cycles * cycles
        return slot // count, source // columns, source % columns // cycles

    shape = (orders, LANES)
    own_order = origin(iota(shape, 1))[2] == iota(shape, 0)
    values = []
    for z in range(bands):
        total = got_ref[z]
        for p in range(1, groups):
            total = total + got_ref[p * bands + z]
        values.append(jnp.where(own_order, jnp.broadcast_to(total, shape), 0.0))
    shape = (3 * cycles_here * 2, LANES)
    row, lane = iota(shape, 0), iota(shape, 1)
    field, cycle, part = row // (2 * cycles_here), row // 2 % cycles_here, row % 2
    lane_part, table, _ = origin(lane)
    same = jnp.where(lane_part == part, 1.0, 0.0)
    other = jnp.where(lane_part == part, 0.0, jnp.where(part == 0, -1.0, 1.0))
    pick = jnp.where(
        field == 0,
        jnp.where(table <= KAPPA_LOW, same, 0.0),
        jnp.where(field == 1, jnp.where(table == PLUS, same, 0.0), jnp.where(table == MINUS, other, 0.0)),
    )
    values = jnp.concatenate(values, 0)
    high, _ = split(values)
    middle, low = split(values - high.astype(jnp.float32))
    pick = jnp.where(lane % cycles_here == cycle, pick, 0.0).astype(jnp.bfloat16)
    maps = lax.dot_general(
        jnp.concatenate([pick] * 3, 1), jnp.concatenate([high, middle, low], 1), (((1,), (1,)), ((), ())),
        preferred_element_type=jnp.float32,
    )
    for i in range(3 * cycles_here):
        out_ref[i] = maps[2 * i : 2 * i + 2]


def on_device(
    cycle_modes, cycle_weight, legendre, spin_plus, spin_minus, window, lensing, source_shell
):
    bands = lax.axis_size("band")
    shell_parts = lax.axis_size("shell")
    shells, cycles_here, _, orders_all = cycle_modes.shape
    orders, cycles, degrees = legendre.shape
    bins = source_shell.shape[0]
    assert bins == shell_parts and 8 * orders * cycles_here == LANES
    offsets = tuple(range(1, bands)) if bands == len(ROUTES) else ()
    rows = 2 * bins
    columns = 4 * orders * cycles

    def shaped(*shape, dtype=jnp.float32):
        return jax.ShapeDtypeStruct(shape, dtype)

    def left_scratch(blocks):
        return [
            pltpu.VMEM((orders * blocks * cycles_here * rows, 2 * shells), jnp.bfloat16),
            pltpu.VMEM((orders * blocks * cycles_here * rows, shells), jnp.bfloat16),
        ]

    block_shape = (cycles_here, 2 * orders, shells)
    out_shape = [shaped(*block_shape)] * bands if offsets else [shaped(bands, *block_shape)]
    out_shape = [*out_shape, shaped(rows, shells)]
    sources = (
        cycle_modes.transpose(1, 2, 3, 0), cycle_weight.reshape(1, cycles_here),
        source_shell.reshape(1, bins), lensing.reshape(1, shells),
    )
    sources = pl.pallas_call(
        load_kernel,
        in_specs=[HBM] * 4,
        out_specs=[VMEM] * 4,
        out_shape=[shaped(*x.shape, dtype=x.dtype) for x in sources],
        scratch_shapes=[pltpu.SemaphoreType.DMA((4,))],
        compiler_params=PARAMS,
        name="load",
    )(*map(keep, sources))
    *blocks, efficiency = pl.pallas_call(
        functools.partial(pack_kernel, bands=bands, orders=orders, bins=bins, offsets=offsets),
        in_specs=[VMEM] * 4,
        out_specs=[VMEM] * len(out_shape),
        out_shape=out_shape,
        scratch_shapes=[pltpu.VMEM((bands, *block_shape), jnp.float32)],
        compiler_params=PARAMS,
        cost_estimate=pl.CostEstimate(flops=10**10, bytes_accessed=2**17, transcendentals=0),
        name="pack",
    )(*sources)
    if offsets:
        own, *sends = blocks
        got = [
            lax.ppermute(send, "band", [(z, ROUTES[k][z]) for z in range(bands)])
            for k, send in zip(offsets, sends)
        ]
    else:
        got = [lax.all_to_all(blocks[0], "band", split_axis=0, concat_axis=0, tiled=True)]
    half = jnp.bfloat16
    tables = [shaped(shells, degrees, dtype=half)] * 2 + [shaped(degrees, columns, dtype=half)]
    binned_shape = shaped(orders * rows, degrees)
    arguments = [window, legendre, spin_plus, spin_minus]
    if offsets:
        tables.append(binned_shape)
        arguments += [efficiency, own]
    high, low, turned, *binned = pl.pallas_call(
        functools.partial(prepare_kernel, orders=orders, cycles_here=cycles_here),
        in_specs=[VMEM] * len(arguments),
        out_specs=[VMEM] * len(tables),
        out_shape=tables,
        scratch_shapes=left_scratch(1) if offsets else [],
        compiler_params=PARAMS,
        name="prepare",
    )(*arguments)
    for k, block in zip(offsets[:-1], got):
        binned = [
            pl.pallas_call(
                functools.partial(more_kernel, orders=orders, cycles_here=cycles_here, offset=k),
                in_specs=[VMEM] * 6,
                out_specs=VMEM,
                out_shape=binned_shape,
                scratch_shapes=left_scratch(1),
                compiler_params=PARAMS,
                name="more",
            )(efficiency, legendre, high, low, *binned, block)
        ]
    last = got[-1:]
    operands = [efficiency, legendre, high, low, turned, *binned, *last]
    maps = pl.pallas_call(
        functools.partial(
            maps_kernel, bands=bands, orders=orders, cycles_here=cycles_here, offsets=offsets[-1:]
        ),
        in_specs=[VMEM] * len(operands),
        out_specs=VMEM,
        out_shape=shaped(bins * bands, 1, LANES),
        scratch_shapes=[
            *left_scratch(len(last) if offsets else bands),
            pltpu.VMEM((3 * orders * rows, columns), jnp.float32),
        ],
        compiler_params=PARAMS,
        name="maps",
    )(*operands)
    got = lax.all_to_all(maps, ("shell", "band"), split_axis=0, concat_axis=0, tiled=True)
    out = pl.pallas_call(
        functools.partial(unpack_kernel, bands=bands, orders=orders, cycles_here=cycles_here),
        in_specs=[VMEM],
        out_specs=VMEM,
        out_shape=shaped(3 * cycles_here, 2, orders_all),
        compiler_params=PARAMS,
        name="unpack",
    )(got)
    return out.reshape(1, 3, cycles_here, 2, orders_all)


def solution(mesh):
    placed = (
        P(("cosmo", "shell"), "band", None, None),
        P("band"),
        P("band", None, None),
        P("band", None, None),
        P("band", None, None),
        P("shell", None),
        P(("cosmo", "shell")),
        P("cosmo"),
    )
    return jax.shard_map(
        on_device,
        mesh=mesh,
        in_specs=placed,
        out_specs=P(("cosmo", "shell"), None, "band", None, None),
        check_vma=False,
    )
```

```python
import functools

import jax
import jax.numpy as jnp
from jax import lax
from jax.experimental import pallas as pl
from jax.experimental.pallas import tpu as pltpu
from jax.sharding import PartitionSpec as P

TILE = 256
GROUP = 16
LANES = 128
ROUTES = ((0, 1, 2, 3), (2, 3, 1, 0), (1, 0, 3, 2), (3, 2, 0, 1))
VMEM = pl.BlockSpec(memory_space=pltpu.VMEM)
HBM = pl.BlockSpec(memory_space=pltpu.HBM)
PARAMS = pltpu.CompilerParams(vmem_limit_bytes=28 * 2**20)
KAPPA_HIGH, KAPPA_LOW, PLUS, MINUS = range(4)


def keep(x):
    return pltpu.with_memory_space_constraint(x, pltpu.HBM)


def route(k, here, back=False):
    ends = tuple(ROUTES[k].index(z) for z in range(4)) if back else ROUTES[k]
    end = jnp.int32(ends[0])
    for z in range(1, 4):
        end = jnp.where(here == z, ends[z], end)
    return end


def split(x):
    high = x.astype(jnp.bfloat16)
    low = (x - high.astype(jnp.float32)).astype(jnp.bfloat16)
    return high, low


def iota(shape, axis):
    return lax.broadcasted_iota(jnp.int32, shape, axis)


def load_kernel(*refs):
    count = len(refs) // 2
    copies = [pltpu.make_async_copy(refs[i], refs[count + i], refs[-1].at[i]) for i in range(count)]
    for copy in copies:
        copy.start()
    for copy in copies:
        copy.wait()


def pack_kernel(modes_ref, weight_ref, *refs, bands, orders, offsets):
    *out_refs, blocks_ref = refs
    cycles_here, _, _, shells = modes_ref.shape
    for r in range(cycles_here):
        weight = jnp.broadcast_to(weight_ref[0:1, r : r + 1], (orders, shells))
        for c in range(2):
            for z in range(bands):
                blocks_ref[z, r, c * orders : (c + 1) * orders, :] = (
                    modes_ref[r, c, z * orders : (z + 1) * orders, :] * weight
                )
    if offsets:
        here = lax.axis_index("band")
        for k, out_ref in zip((0, *offsets), out_refs):
            out_ref[...] = blocks_ref[route(k, here)]
    else:
        out_refs[0][...] = blocks_ref[...]


def efficiency_of(source_ref, lensing_ref, bins):
    shells = lensing_ref.shape[1]
    rows = 2 * bins
    row_bin = iota((rows, shells), 0) % bins
    source = jnp.zeros((rows, shells), jnp.int32)
    for b in range(bins):
        source = jnp.where(row_bin == b, jnp.broadcast_to(source_ref[0:1, b : b + 1], (rows, shells)), source)
    shell_ids = lax.axis_index("shell") * shells + iota((rows, shells), 1)
    return (
        lensing_ref[...]
        * jnp.maximum(source - shell_ids, 0).astype(jnp.float32)
        / (source + 1).astype(jnp.float32)
    )


def left_of(modes, efficiency, orders, bins):
    cycles, _, shells = modes.shape
    rows = 2 * bins
    first_part = (iota((1, rows, shells), 1) < bins)
    parts = []
    for m in range(orders):
        real = jnp.broadcast_to(modes[:, m : m + 1, :], (cycles, rows, shells))
        imag = jnp.broadcast_to(modes[:, orders + m : orders + m + 1, :], (cycles, rows, shells))
        left = jnp.where(first_part, real, imag) * efficiency[None]
        parts.append(left.reshape(cycles * rows, shells))
    high, low = split(jnp.concatenate(parts, 0))
    return jnp.concatenate([high, low], 1), high


def multiply(left, left_high, high, low):
    product = jnp.dot(left, jnp.concatenate([high, high], 0), preferred_element_type=jnp.float32)
    return product + jnp.dot(left_high, low, preferred_element_type=jnp.float32)


def add_cycles(binned, product, legendre_ref, firsts, lanes, orders, rows):
    out = []
    at = 0
    for m in range(orders):
        total = binned[m]
        for first, count in firsts:
            for r in range(count):
                total = total + legendre_ref[m, pl.ds(first + r, 1), lanes] * product[at : at + rows]
                at += rows
        out.append(total)
    return out


def each_tile(degrees, unroll, step, size=TILE):
    if unroll:
        for start in range(0, degrees, size):
            step(start)
    else:
        pl.loop(0, degrees // size)(lambda i: step(pl.multiple_of(i * size, size)))


def gather_left(modes_refs, efficiency_ref, left_ref, left_high_ref, orders, cycles_here, offsets):
    if offsets:
        here = lax.axis_index("band")
        firsts = [(route(k, here, True) * cycles_here, cycles_here) for k in offsets]
        modes = jnp.concatenate([ref[...] for ref in modes_refs], 0)
    else:
        modes = modes_refs[0][...]
        modes = modes.reshape(-1, *modes.shape[2:])
        firsts = [(0, modes.shape[0])]
    left_ref[...], left_high_ref[...] = left_of(
        modes, efficiency_ref[...], orders, efficiency_ref.shape[0] // 2
    )
    return firsts


def prepare_kernel(
    source_ref, lensing_ref, window_ref, legendre_ref, plus_ref, minus_ref, *refs, orders, cycles_here,
):
    own = len(refs) > 4
    if own:
        own_ref, *refs, binned_ref, left_ref, left_high_ref = refs
    efficiency_ref, high_ref, low_ref, tables_ref = refs
    rows = efficiency_ref.shape[0]
    efficiency_ref[...] = efficiency_of(source_ref, lensing_ref, rows // 2)
    if own:
        firsts = gather_left([own_ref], efficiency_ref, left_ref, left_high_ref, orders, cycles_here, (0,))
    columns = legendre_ref.shape[0] * legendre_ref.shape[1]
    same = jnp.where(iota((TILE, TILE), 0) == iota((TILE, TILE), 1), 1.0, 0.0).astype(jnp.bfloat16)

    def step(start):
        lanes = pl.ds(start, TILE)
        high, low = split(window_ref[:, lanes])
        high_ref[:, lanes], low_ref[:, lanes] = high, low
        tables = [
            *split(legendre_ref[:, :, lanes].reshape(columns, TILE)),
            plus_ref[:, :, lanes].reshape(columns, TILE),
            minus_ref[:, :, lanes].reshape(columns, TILE),
        ]
        tables_ref[lanes, :] = lax.dot_general(
            same, jnp.concatenate(tables, 0), (((1,), (1,)), ((), ())), preferred_element_type=jnp.float32,
        ).astype(jnp.bfloat16)
        if own:
            binned = add_cycles(
                [jnp.zeros((rows, TILE), jnp.float32)] * orders,
                multiply(left_ref[...], left_high_ref[...], high, low), legendre_ref, firsts, lanes, orders, rows,
            )
            for m in range(orders):
                binned_ref[pl.ds(m * rows, rows), lanes] = binned[m]

    each_tile(legendre_ref.shape[2], own, step)


def more_kernel(
    efficiency_ref, legendre_ref, high_ref, low_ref, binned_in, *refs, orders, cycles_here, offsets,
):
    *modes_refs, binned_ref, left_ref, left_high_ref = refs
    rows = efficiency_ref.shape[0]
    firsts = gather_left(modes_refs, efficiency_ref, left_ref, left_high_ref, orders, cycles_here, offsets)

    def step(start):
        lanes = pl.ds(start, TILE)
        binned = add_cycles(
            [binned_in[pl.ds(m * rows, rows), lanes] for m in range(orders)],
            multiply(left_ref[...], left_high_ref[...], high_ref[:, lanes], low_ref[:, lanes]),
            legendre_ref, firsts, lanes, orders, rows,
        )
        for m in range(orders):
            binned_ref[pl.ds(m * rows, rows), lanes] = binned[m]

    each_tile(legendre_ref.shape[2], True, step)


def maps_kernel(
    efficiency_ref, legendre_ref, high_ref, low_ref, tables_ref, *refs,
    bands, orders, cycles_here, offsets,
):
    if offsets:
        binned_ref, *refs = refs
    *modes_refs, out_ref, left_ref, left_high_ref, sums_ref = refs
    cycles = legendre_ref.shape[1]
    rows = efficiency_ref.shape[0]
    bins = rows // 2
    columns = orders * cycles
    firsts = gather_left(modes_refs, efficiency_ref, left_ref, left_high_ref, orders, cycles_here, offsets)
    sums_ref[...] = jnp.zeros(sums_ref.shape, jnp.float32)

    group = GROUP if offsets else 2

    def coefficients(start, product):
        lanes = pl.ds(start, TILE)
        if offsets:
            binned = [binned_ref[pl.ds(m * rows, rows), lanes] for m in range(orders)]
        else:
            binned = [jnp.zeros((rows, TILE), jnp.float32)] * orders
        binned = add_cycles(binned, product, legendre_ref, firsts, lanes, orders, rows)
        binned = jnp.concatenate(binned, 0)
        degree = (start + iota((rows, TILE), 1)).astype(jnp.float32)
        ratio = jnp.where(
            degree >= 2.0,
            jnp.sqrt((degree + 2.0) * (degree - 1.0) / jnp.maximum(degree * (degree + 1.0), 1.0)),
            0.0,
        )
        shear = (-jnp.concatenate([ratio] * orders, 0) * binned).astype(jnp.bfloat16)
        high, low = split(binned)
        return jnp.concatenate([high, low, shear], 0)

    def step(start):
        starts = [start + i * TILE for i in range(group)]
        spans = [pl.ds(at, TILE) for at in starts]
        products = [
            multiply(left_ref[...], left_high_ref[...], high_ref[:, lanes], low_ref[:, lanes]) for lanes in spans
        ]
        lefts = [coefficients(*pair) for pair in zip(starts, products)]
        parts = [
            jnp.dot(left, tables_ref[lanes, :], preferred_element_type=jnp.float32)
            for left, lanes in zip(lefts, spans)
        ]
        sums_ref[...] += sum(parts[1:], parts[0])

    each_tile(legendre_ref.shape[2], bool(offsets), step, group * TILE)

    lane = iota((rows, 4 * columns), 1)
    table = lane // columns
    order = lane % columns // cycles

    def own(kind):
        total = jnp.zeros((rows, 4 * columns), jnp.float32)
        for m in range(orders):
            total = jnp.where(order == m, sums_ref[pl.ds((kind * orders + m) * rows, rows), :], total)
        return total

    kappa = own(0) + jnp.where(table == KAPPA_HIGH, own(1), 0.0)
    value = jnp.where(table < PLUS, kappa, own(2))
    count = 4 * columns // LANES
    slot = iota((rows, LANES), 1) % cycles // cycles_here
    shifted = {}
    for z in range(bands):
        halves = []
        for c in range(2):
            half = jnp.zeros((rows, LANES), jnp.float32)
            for v in range(count):
                at = c * count + v
                shift = (at - z) * cycles_here % LANES
                if (v, shift) not in shifted:
                    part = value[:, v * LANES : (v + 1) * LANES]
                    shifted[v, shift] = pltpu.roll(part, shift, 1) if shift else part
                half = jnp.where(slot == at, shifted[v, shift], half)
            halves.append(half)
        row = jnp.where(slot[:bins] < count, halves[0][:bins], halves[1][bins:])
        for b in range(bins):
            out_ref[b * bands + z] = row[b : b + 1]


def unpack_kernel(got_ref, out_ref, *, bands, orders, cycles_here):
    groups = got_ref.shape[0] // bands
    cycles = bands * cycles_here
    columns = orders * cycles
    count = 4 * columns // LANES

    def origin(lane):
        slot = lane % cycles // cycles_here
        source = slot % count * LANES + lane // cycles * cycles
        return slot // count, source // columns, source % columns // cycles

    shape = (orders, LANES)
    own_order = origin(iota(shape, 1))[2] == iota(shape, 0)
    values = []
    for z in range(bands):
        total = got_ref[z]
        for p in range(1, groups):
            total = total + got_ref[p * bands + z]
        values.append(jnp.where(own_order, jnp.broadcast_to(total, shape), 0.0))
    shape = (3 * cycles_here * 2, LANES)
    row, lane = iota(shape, 0), iota(shape, 1)
    field, cycle, part = row // (2 * cycles_here), row // 2 % cycles_here, row % 2
    lane_part, table, _ = origin(lane)
    same = jnp.where(lane_part == part, 1.0, 0.0)
    other = jnp.where(lane_part == part, 0.0, jnp.where(part == 0, -1.0, 1.0))
    pick = jnp.where(
        field == 0,
        jnp.where(table <= KAPPA_LOW, same, 0.0),
        jnp.where(field == 1, jnp.where(table == PLUS, same, 0.0), jnp.where(table == MINUS, other, 0.0)),
    )
    maps = lax.dot_general(
        jnp.where(lane % cycles_here == cycle, pick, 0.0), jnp.concatenate(values, 0), (((1,), (1,)), ((), ())),
        precision=lax.Precision.HIGHEST, preferred_element_type=jnp.float32,
    )
    for i in range(3 * cycles_here):
        out_ref[i] = maps[2 * i : 2 * i + 2]


def on_device(
    cycle_modes, cycle_weight, legendre, spin_plus, spin_minus, window, lensing, source_shell
):
    bands = lax.axis_size("band")
    shell_parts = lax.axis_size("shell")
    shells, cycles_here, _, orders_all = cycle_modes.shape
    orders, cycles, degrees = legendre.shape
    bins = source_shell.shape[0]
    assert bins == shell_parts and 8 * orders * cycles_here == LANES
    offsets = (1, 2, 3) if bands == 4 else ()
    rows = 2 * bins
    columns = 4 * orders * cycles

    def shaped(*shape, dtype=jnp.float32):
        return jax.ShapeDtypeStruct(shape, dtype)

    def left_scratch(blocks):
        return [
            pltpu.VMEM((orders * blocks * cycles_here * rows, 2 * shells), jnp.bfloat16),
            pltpu.VMEM((orders * blocks * cycles_here * rows, shells), jnp.bfloat16),
        ]

    block_shape = (cycles_here, 2 * orders, shells)
    out_shape = [shaped(*block_shape)] * bands if offsets else [shaped(bands, *block_shape)]
    sources = cycle_modes.transpose(1, 2, 3, 0), cycle_weight.reshape(1, cycles_here)
    sources = pl.pallas_call(
        load_kernel,
        in_specs=[HBM] * 2,
        out_specs=[VMEM] * 2,
        out_shape=[shaped(*x.shape) for x in sources],
        scratch_shapes=[pltpu.SemaphoreType.DMA((2,))],
        compiler_params=PARAMS,
        name="load",
    )(*map(keep, sources))
    blocks = pl.pallas_call(
        functools.partial(pack_kernel, bands=bands, orders=orders, offsets=offsets),
        in_specs=[VMEM] * 2,
        out_specs=[VMEM] * len(out_shape),
        out_shape=out_shape,
        scratch_shapes=[pltpu.VMEM((bands, *block_shape), jnp.float32)],
        compiler_params=PARAMS,
        cost_estimate=pl.CostEstimate(flops=10**10, bytes_accessed=2**17, transcendentals=0),
        name="pack",
    )(*sources)
    if offsets:
        own, *sends = blocks
        got = [
            lax.ppermute(send, "band", [(z, ROUTES[k][z]) for z in range(bands)])
            for k, send in zip(offsets, sends)
        ]
    else:
        got = [lax.all_to_all(blocks[0], "band", split_axis=0, concat_axis=0, tiled=True)]
    half = jnp.bfloat16
    tables = [shaped(rows, shells)] + [shaped(shells, degrees, dtype=half)] * 2 + [shaped(degrees, columns, dtype=half)]
    binned_shape = shaped(orders * rows, degrees)
    arguments = [
        source_shell.reshape(1, bins), lensing.reshape(1, shells), window, legendre, spin_plus, spin_minus,
    ]
    if offsets:
        tables.append(binned_shape)
        arguments.append(own)
    efficiency, high, low, turned, *binned = pl.pallas_call(
        functools.partial(prepare_kernel, orders=orders, cycles_here=cycles_here),
        in_specs=[VMEM] * len(arguments),
        out_specs=[VMEM] * len(tables),
        out_shape=tables,
        scratch_shapes=left_scratch(1) if offsets else [],
        compiler_params=PARAMS,
        name="prepare",
    )(*arguments)
    if offsets:
        early = got[:-1]
        binned = [
            pl.pallas_call(
                functools.partial(more_kernel, orders=orders, cycles_here=cycles_here, offsets=offsets[:-1]),
                in_specs=[VMEM] * (5 + len(early)),
                out_specs=VMEM,
                out_shape=binned_shape,
                scratch_shapes=left_scratch(len(early)),
                compiler_params=PARAMS,
                name="more",
            )(efficiency, legendre, high, low, *binned, *early)
        ]
    last = got[-1:]
    operands = [efficiency, legendre, high, low, turned, *binned, *last]
    maps = pl.pallas_call(
        functools.partial(
            maps_kernel, bands=bands, orders=orders, cycles_here=cycles_here, offsets=offsets[-1:]
        ),
        in_specs=[VMEM] * len(operands),
        out_specs=VMEM,
        out_shape=shaped(bins * bands, 1, LANES),
        scratch_shapes=[
            *left_scratch(len(last) if offsets else bands),
            pltpu.VMEM((3 * orders * rows, columns), jnp.float32),
        ],
        compiler_params=PARAMS,
        name="maps",
    )(*operands)
    got = lax.all_to_all(maps, ("shell", "band"), split_axis=0, concat_axis=0, tiled=True)
    out = pl.pallas_call(
        functools.partial(unpack_kernel, bands=bands, orders=orders, cycles_here=cycles_here),
        in_specs=[VMEM],
        out_specs=VMEM,
        out_shape=shaped(3 * cycles_here, 2, orders_all),
        compiler_params=PARAMS,
        name="unpack",
    )(got)
    return out.reshape(1, 3, cycles_here, 2, orders_all)


def solution(mesh):
    placed = (
        P(("cosmo", "shell"), "band", None, None),
        P("band"),
        P("band", None, None),
        P("band", None, None),
        P("band", None, None),
        P("shell", None),
        P(("cosmo", "shell")),
        P("cosmo"),
    )
    return jax.shard_map(
        on_device,
        mesh=mesh,
        in_specs=placed,
        out_specs=P(("cosmo", "shell"), None, "band", None, None),
        check_vma=False,
    )
```
